128 devices in a mesh: grp: 4 (over y), vir: 32 (over x, z, core).
Axes of the slice: x: 4, y: 4, z: 4, core: 2. Of those that a mesh axis runs over, the one named last changes fastest.
Arguments:
- triplets: int32 [24, 3], P('grp'), may hold values from 0 to 4, as said below
- counts: int32 [4], P('grp'), may hold values from 1 to 6, as said below
- weights: int32 [24], P('grp'), may hold values from 1 to 3
- a_pick: int32 [64], P('vir'), may hold values from 0 to 895, as said below
- occ_energy: float32 [5], replicated, may hold values from -2 to -0.5
- vir_energy: float32 [896], replicated, may hold values from 0.3 to 3
- ints_vvvo: bfloat16 [5, 64, 896, 896], P(None, 'vir'), may hold values from -0.1875 to 0.1875
- t2pair: bfloat16 [5, 5, 896, 896], P(None, None, 'vir'), may hold values from -6 to 6
- t2hole: bfloat16 [5, 60, 64, 896], P(None, None, 'vir'), may hold values from -6 to 6
- ints_hole: bfloat16 [5, 5, 60, 896], replicated, may hold values from -0.75 to 0.75
Outputs:
- trip_energy: float32 [24], P('grp')
- orbital_energy: float32 [64], P('vir')
The draws below stay inside these ranges and needn't reach their ends.
Inputs may be any that keep to these rules, and one draw needn't show every extreme that they name: `triplets`: each row holds occupied indices i <= j <= k. `counts`: some group has all 6 slots live. `a_pick`: the entries are distinct.
All inputs are finite; a program needn't handle non-finite values.
Results may differ from the reference program's by a relative error of at most 0.0003.
Values may be sent and summed in bfloat16 or wider, within the bound.
A program may use at most 64 MiB of HBM per device.

```python
import math
import jax
import jax.numpy as jnp
from jax import lax

V = 896
O = 60
OW = 5
NT = 6
GROUPS = 4
TRIPLETS = 24
AW = 64


def draw_triplets(key, part):
    values = jax.random.randint(key, (TRIPLETS, 3), 0, OW)
    return jnp.sort(values, axis=1).astype(jnp.int32)


def draw_counts(key, part):
    filled = jax.random.randint(jax.random.fold_in(key, 11), (GROUPS,), 1, NT + 1)
    chosen = jax.random.randint(jax.random.fold_in(key, 12), (), 0, GROUPS)
    groups_iota = jnp.arange(GROUPS, dtype=jnp.int32)
    return jnp.where(groups_iota == chosen, NT, filled).astype(jnp.int32)


def draw_a_pick(key, part):
    order = jax.random.permutation(jax.random.fold_in(key, 21), V)
    return order[:AW].astype(jnp.int32)


def with_ends(array, stream_key, least, top_value):
    extent = array.shape
    place = [jax.random.randint(jax.random.fold_in(stream_key, axis), (), 0, extent[axis]) for axis in range(len(extent))]
    array = array.at[tuple(place)].set(least)
    longest = extent.index(max(extent))
    place[longest] = (place[longest] + 1) % extent[longest]
    return array.at[tuple(place)].set(top_value)


def block_scale(own_key, extent, cuts, least, largest):
    level = 1.0
    for dim, parts in cuts:
        heights = jax.random.uniform(jax.random.fold_in(jax.random.fold_in(own_key, 6), dim), (parts,), jnp.float32, least / len(cuts), largest / len(cuts))
        level = level * jnp.repeat(jnp.exp(heights), extent[dim] // parts).reshape((-1,) + (1,) * (len(extent) - 1 - dim))
    return level


def scatter_about(key, shape, scale, reach, pieces=(), kind=jnp.bfloat16):
    values = scale * jax.random.normal(key, shape, jnp.float32)
    if pieces:
        values = values * block_scale(key, shape, pieces, -0.22, 0.18)
    return jnp.clip(values, -reach, reach).astype(kind)


def setup_inputs(seed: int = 0) -> dict:
    key_of = jax.random.split(jax.random.key(seed), 11)
    triplets = draw_triplets(jax.random.fold_in(key_of[10], 71), 0)
    counts = draw_counts(jax.random.fold_in(key_of[10], 71), 0)
    weights = with_ends(jax.random.randint(key_of[2], (TRIPLETS,), 1, 4), jax.random.fold_in(key_of[2], 1), 1, 3).astype(jnp.int32)
    a_pick = draw_a_pick(jax.random.fold_in(key_of[10], 71), 0)
    occ_energy = jnp.clip(jax.random.uniform(key_of[4], (OW,), jnp.float32, -2.0, -0.5), -2.0, -0.5)
    vir_energy = jnp.clip(jnp.exp(jax.random.uniform(key_of[5], (V,), jnp.float32, math.log(0.3), math.log(3.0))), 0.3, 3.0)
    ints_vvvo = scatter_about(key_of[6], (OW, AW, V, V), V ** -0.5, 0.1875, ((1, 32),))
    t2pair = scatter_about(key_of[7], (OW, OW, V, V), 1.0, 6.0, ((2, 32),))
    t2hole = scatter_about(key_of[8], (OW, O, AW, V), 1.0, 6.0, ((2, 32),))
    ints_hole = scatter_about(key_of[9], (OW, OW, O, V), O ** -0.5, 0.75)
    return dict(triplets=triplets, counts=counts, weights=weights, a_pick=a_pick, occ_energy=occ_energy, vir_energy=vir_energy, ints_vvvo=ints_vvvo, t2pair=t2pair, t2hole=t2hole, ints_hole=ints_hole)


def reference(triplets, counts, weights, a_pick, occ_energy, vir_energy, ints_vvvo, t2pair, t2hole, ints_hole):
    a_energy = vir_energy[a_pick]
    width = vir_energy.shape[0]
    window = a_pick.shape[0]

    def one_slot(orbital, slot_index):
        trip_row = triplets[slot_index]
        occ_i = trip_row[0]
        occ_j = trip_row[1]
        occ_k = trip_row[2]
        integral_slab = ints_vvvo[occ_k].astype(jnp.float32)
        pair_slab = t2pair[occ_j, occ_k].astype(jnp.float32)
        hole_amps = t2hole[occ_i].astype(jnp.float32)
        hole_ints = ints_hole[occ_k, occ_j].astype(jnp.float32)
        particle = jnp.einsum('abd,cd->abc', integral_slab, pair_slab, precision=lax.Precision.HIGHEST)
        holes_term = jnp.einsum('lab,lc->abc', hole_amps, hole_ints, precision=lax.Precision.HIGHEST)
        amplitude = particle - holes_term
        occ_shift = occ_energy[occ_i] + occ_energy[occ_j] + occ_energy[occ_k]
        denominator = a_energy[:, None, None] + vir_energy[None, :, None] + vir_energy[None, None, :] - occ_shift
        live = (slot_index % NT) < counts[slot_index // NT]
        factor = jnp.where(live, -weights[slot_index].astype(jnp.float32) / (width * width), jnp.float32(0.0))
        energy = factor * jnp.sum(amplitude * amplitude / denominator, axis=(1, 2))
        return orbital + energy, jnp.sum(energy) / window

    orbital, trip_energy = lax.scan(one_slot, jnp.zeros((window,), jnp.float32), jnp.arange(TRIPLETS, dtype=jnp.int32))
    return trip_energy, orbital
```

```python
import jax
import jax.numpy as jnp
from jax import lax
from jax.experimental import pallas as pl
from jax.experimental.pallas import tpu as pltpu
from jax.sharding import PartitionSpec as P

V = 896
BLOCK = 28
ROWS = 32
PAIRS = 15
OW = 5
LEAD = 2
CHUNK = 224
NT_DIMS = (((1,), (1,)), ((), ()))


def pair_of(step):
    q = PAIRS - 1 - step
    k = (
        (q >= 1).astype(jnp.int32)
        + (q >= 3).astype(jnp.int32)
        + (q >= 6).astype(jnp.int32)
        + (q >= 10).astype(jnp.int32)
    )
    return q, q - k * (k + 1) // 2, k


def kernel(
    t2_ref, vvvo_ref, th_ref, ih_ref, yc_ref, xb_ref, occ_ref, e_ref,
    src, slab, vv, wbuf, send1, recv1, send2, recv2, send3, recv3, vsem,
):
    y = lax.axis_index("grp")
    vir = lax.axis_index("vir")
    core = vir % 2
    x = vir // 8
    z = (vir // 2) % 4

    def place(p):
        is_a = (p % 2) == 0
        u = jnp.where(is_a, x, z)
        w = jnp.where(is_a, z, x)
        off = (y + p // 2) % 4
        return is_a, u, w, off

    def device(is_a, u, w):
        return {"vir": jnp.where(is_a, u * 8 + w * 2, w * 8 + u * 2) + core}

    def first(p):
        is_a, u, w, off = place(p)
        return pltpu.make_async_remote_copy(
            src_ref=src.at[p],
            dst_ref=slab.at[p, core, w],
            send_sem=send1.at[p],
            recv_sem=recv1.at[p],
            device_id=device(is_a, (u + 4 - off) % 4, w),
            device_id_type=pl.DeviceIdType.MESH,
        ), off

    def second(p, turn):
        is_a, u, w, off = place(p)
        shift = (1, 3, 2)[turn]
        return pltpu.make_async_remote_copy(
            src_ref=slab.at[p, core, w],
            dst_ref=slab.at[p, core, w],
            send_sem=send2.at[p, turn],
            recv_sem=recv2.at[p, turn],
            device_id=device(is_a, u, (w + shift) % 4),
            device_id_type=pl.DeviceIdType.MESH,
        )

    def third(p):
        return pltpu.make_async_remote_copy(
            src_ref=slab.at[p, core],
            dst_ref=slab.at[p, core],
            send_sem=send3.at[p],
            recv_sem=recv3.at[p],
            device_id={"vir": vir + 1 - 2 * core},
            device_id_type=pl.DeviceIdType.MESH,
        )

    def load(k):
        return pltpu.make_async_copy(vvvo_ref.at[k], vv.at[k], vsem.at[k])

    barrier = pltpu.get_barrier_semaphore()
    for shift in (1, 2, 3):
        pl.semaphore_signal(
            barrier, inc=1, device_id={"vir": (((x + shift) % 4) * 4 + z) * 2 + core},
            device_id_type=pl.DeviceIdType.MESH)
        pl.semaphore_signal(
            barrier, inc=1, device_id={"vir": (x * 4 + (z + shift) % 4) * 2 + core},
            device_id_type=pl.DeviceIdType.MESH)
    pl.semaphore_signal(
        barrier, inc=1, device_id={"vir": vir + 1 - 2 * core},
        device_id_type=pl.DeviceIdType.MESH)

    for k in range(OW - 1, -1, -1):
        load(k).start()

    def fill(p, carry):
        q, j, k = pair_of(p)
        is_a, u, w, off = place(p)
        block = t2_ref[j, k]
        src[p, BLOCK - 12:, :] = jnp.zeros((ROWS - BLOCK + 12, V), jnp.bfloat16)
        src[p, :BLOCK, :] = block

        @pl.when(off == 0)
        def _():
            slab[p, core, w, BLOCK - 12:, :] = jnp.zeros((ROWS - BLOCK + 12, V), jnp.bfloat16)
            slab[p, core, w, :BLOCK, :] = block

        return carry

    lax.fori_loop(0, PAIRS, fill, 0)
    e_ref[...] = jnp.zeros_like(e_ref)
    pl.semaphore_wait(barrier, 7)

    def start_first(p):
        copy, off = first(p)

        @pl.when(off != 0)
        def _():
            copy.start()

    for p in range(LEAD):
        start_first(p)

    def compute(p):
        q, j, k = pair_of(p)
        is_a, u, w, off = place(p)
        fresh = (p == 0) | (q == (k + 1) * (k + 2) // 2 - 1)

        @pl.when(fresh)
        def _():
            load(k).wait()

        cols = slab[p].reshape(2 * 4 * ROWS, V)
        wbuf[...] = lax.dot_general(vv[k], cols, NT_DIMS, preferred_element_type=jnp.float32)

        row = lax.broadcasted_iota(jnp.int32, (256, 1), 0)
        r_core = row // 128
        r_w = (row // ROWS) % 4
        r_in = row % ROWS
        source = (u + off) % 4
        owner = jnp.where(is_a, source * 8 + r_w * 2, r_w * 8 + source * 2) + r_core
        target = jnp.where(r_in < BLOCK, owner * BLOCK + r_in, -1)
        column = lax.broadcasted_iota(jnp.int32, (256, V), 1)
        select = (column == target).astype(jnp.float32).astype(jnp.bfloat16)
        holes = lax.dot_general(
            select, ih_ref[k, j], NT_DIMS, preferred_element_type=jnp.float32
        ).astype(jnp.bfloat16)
        variant = jnp.where(is_a, 0, 4) + source
        yc_row = yc_ref[pl.ds(variant, 1), :]

        def one(i, carry):
            shift = occ_ref[i] + occ_ref[j] + occ_ref[k]
            yc = yc_row - shift
            for a in range(2):
                total = jnp.zeros((8, 256), jnp.float32)
                for c in range(V // CHUNK):
                    at = a * V + c * CHUNK
                    hole = lax.dot_general(
                        th_ref[i, at:at + CHUNK, :], holes, NT_DIMS,
                        preferred_element_type=jnp.float32)
                    amp = wbuf[at:at + CHUNK, :] + hole
                    base = xb_ref[at:at + CHUNK, :]
                    den = jnp.concatenate([base, base], axis=1) + yc
                    term = amp * amp / den
                    total = total + jnp.sum(term.reshape(CHUNK // 8, 8, 256), axis=0)
                line = jnp.sum(total, axis=0, keepdims=True)
                line = line[:, :128] + line[:, 128:]
                e_ref[pl.ds((q * OW + i) * 2 + a, 1), :] = line
            return carry

        lax.fori_loop(0, j + 1, one, 0)

    def step(s, carry):
        @pl.when(s + LEAD < PAIRS)
        def _():
            start_first(s + LEAD)

        @pl.when(s < PAIRS)
        def _():
            copy, off = first(s)

            @pl.when(off != 0)
            def _():
                copy.wait_recv()

            for turn in range(3):
                second(s, turn).start()

        @pl.when((s >= 1) & (s < PAIRS + 1))
        def _():
            for turn in range(3):
                second(s - 1, turn).wait_recv()
            third(s - 1).start()

        @pl.when(s >= 2)
        def _():
            third(s - 2).wait_recv()
            compute(s - 2)

        return carry

    lax.fori_loop(0, PAIRS + 2, step, 0)

    def drain(p, carry):
        copy, off = first(p)

        @pl.when(off != 0)
        def _():
            copy.wait_send()

        for turn in range(3):
            second(p, turn).wait_send()
        third(p).wait_send()
        return carry

    lax.fori_loop(0, PAIRS, drain, 0)


def from_everyone(value, axis):
    length = lax.axis_size(axis)
    return lax.all_to_all(
        jnp.broadcast_to(value[None], (length, *value.shape)), axis, 0, 0, tiled=True
    )


def over_copies(value, axis):
    return jnp.sum(from_everyone(value, axis), axis=0)


def pick_energy(a_pick, vir_energy):
    columns = jnp.arange(vir_energy.shape[0], dtype=jnp.int32)
    return jnp.sum(jnp.where(a_pick[:, None] == columns[None, :], vir_energy[None, :], 0.0), axis=1)


def tables(a_pick, vir_energy, t2hole):
    e_a = pick_energy(a_pick, vir_energy)
    base = (e_a[:, None] + vir_energy[None, :]).reshape(2 * V, 1)
    xb = jnp.broadcast_to(base, (2 * V, 128))
    split = vir_energy.reshape(4, 4, 2, BLOCK)
    split = jnp.pad(split, ((0, 0), (0, 0), (0, 0), (0, ROWS - BLOCK)), constant_values=1.0)
    by_x = jnp.transpose(split, (0, 2, 1, 3)).reshape(4, 256)
    by_z = jnp.transpose(split, (1, 2, 0, 3)).reshape(4, 256)
    yc = jnp.concatenate([by_x, by_z], axis=0)
    th = -jnp.transpose(t2hole, (0, 2, 3, 1)).reshape(OW, 2 * V, 60)
    return xb, yc, th


def partial_energies(t2pair, ints_vvvo, th, ints_hole, yc, xb, occ_energy):
    vmem = pl.BlockSpec(memory_space=pltpu.VMEM)
    return pl.pallas_call(
        kernel,
        out_shape=jax.ShapeDtypeStruct((160, 128), jnp.float32),
        in_specs=[
            vmem, pl.BlockSpec(memory_space=pl.ANY), vmem, vmem, vmem, vmem,
            pl.BlockSpec(memory_space=pltpu.SMEM),
        ],
        out_specs=vmem,
        scratch_shapes=[
            pltpu.VMEM((PAIRS, ROWS, V), jnp.bfloat16),
            pltpu.VMEM((PAIRS, 2, 4, ROWS, V), jnp.bfloat16),
            pltpu.VMEM((OW, 2 * V, V), jnp.bfloat16),
            pltpu.VMEM((2 * V, 256), jnp.float32),
            pltpu.SemaphoreType.DMA((PAIRS,)),
            pltpu.SemaphoreType.DMA((PAIRS,)),
            pltpu.SemaphoreType.DMA((PAIRS, 3)),
            pltpu.SemaphoreType.DMA((PAIRS, 3)),
            pltpu.SemaphoreType.DMA((PAIRS,)),
            pltpu.SemaphoreType.DMA((PAIRS,)),
            pltpu.SemaphoreType.DMA((OW,)),
        ],
        compiler_params=pltpu.CompilerParams(
            collective_id=0, has_side_effects=True, vmem_limit_bytes=60 * 1024 * 1024
        ),
    )(t2pair, ints_vvvo.reshape(OW, 2 * V, V), th, ints_hole, yc, xb, occ_energy)


def shards(
    triplets, counts, weights, a_pick, occ_energy, vir_energy, ints_vvvo, t2pair, t2hole, ints_hole
):
    slots = triplets.shape[0]
    window = a_pick.shape[0] * lax.axis_size("vir")
    xb, yc, th = tables(a_pick, vir_energy, t2hole)
    lines = partial_energies(t2pair, ints_vvvo, th, ints_hole, yc, xb, occ_energy)
    cells = PAIRS * OW
    energy = jnp.sum(lines[: cells * 2], axis=1)

    code = (triplets[:, 2] * (triplets[:, 2] + 1) // 2 + triplets[:, 1]) * OW + triplets[:, 0]
    live = jnp.arange(slots, dtype=jnp.int32) < counts[0]
    factor = jnp.where(live, -weights.astype(jnp.float32) / (V * V), 0.0)
    hit = jnp.where(code[:, None] == jnp.arange(cells, dtype=jnp.int32)[None, :], factor[:, None], 0.0)
    total = over_copies(jnp.concatenate([energy, jnp.sum(hit, axis=0)]), "grp")
    whole = total[: cells * 2].reshape(cells, 2)
    orbital = jnp.sum(total[cells * 2 :, None] * whole, axis=0)
    mine = jnp.sum(hit * jnp.sum(whole, axis=1)[None, :], axis=1)
    trip_energy = over_copies(mine, "vir") / window
    return (trip_energy, orbital)


def solution(mesh):
    placed = (
        P("grp", None),
        P("grp"),
        P("grp"),
        P("vir"),
        P(),
        P(),
        P(None, "vir", None, None),
        P(None, None, "vir", None),
        P(None, None, "vir", None),
        P(),
    )
    return jax.shard_map(
        shards, mesh=mesh, in_specs=placed, out_specs=(P("grp"), P("vir")), check_vma=False
    )
```

```python
import jax
import jax.numpy as jnp
from jax import lax
from jax.experimental import pallas as pl
from jax.experimental.pallas import tpu as pltpu
from jax.sharding import PartitionSpec as P

V = 896
BLOCK = 28
ROWS = 32
PAIRS = 15
OW = 5
LEAD = 4
LAG2 = 3
LAG3 = 6
LAG4 = 8
CHUNK = 224
NT_DIMS = (((1,), (1,)), ((), ()))


def pair_of(step):
    q = PAIRS - 1 - step
    k = (
        (q >= 1).astype(jnp.int32)
        + (q >= 3).astype(jnp.int32)
        + (q >= 6).astype(jnp.int32)
        + (q >= 10).astype(jnp.int32)
    )
    return q, q - k * (k + 1) // 2, k


def kernel(
    t2_ref, vvvo_ref, th_ref, ih_ref, yc_ref, xb_ref, hit_ref, occ_ref, trip_ref, orb_ref,
    src, slab, vv, wbuf, send1, recv1, send2, recv2, send3, recv3, vsem,
    tile, ybox, part, vbox, ysend, yrecv, psend, precv,
):
    y = lax.axis_index("grp")
    vir = lax.axis_index("vir")
    core = vir % 2
    x = vir // 8
    z = (vir // 2) % 4

    def place(p):
        is_a = (p % 2) == 0
        u = jnp.where(is_a, x, z)
        w = jnp.where(is_a, z, x)
        off = (y + p // 2) % 4
        return is_a, u, w, off

    def device(is_a, u, w):
        return {"vir": jnp.where(is_a, u * 8 + w * 2, w * 8 + u * 2) + core}

    def first(p):
        is_a, u, w, off = place(p)
        return pltpu.make_async_remote_copy(
            src_ref=src.at[p],
            dst_ref=slab.at[p, core, w],
            send_sem=send1.at[p],
            recv_sem=recv1.at[p],
            device_id=device(is_a, (u + 4 - off) % 4, w),
            device_id_type=pl.DeviceIdType.MESH,
        ), off

    def second(p, turn):
        is_a, u, w, off = place(p)
        shift = (1, 3)[turn]
        return pltpu.make_async_remote_copy(
            src_ref=slab.at[p, core, w],
            dst_ref=slab.at[p, core, w],
            send_sem=send2.at[p, turn],
            recv_sem=recv2.at[p, turn],
            device_id=device(is_a, u, (w + shift) % 4),
            device_id_type=pl.DeviceIdType.MESH,
        )

    def relay(p):
        is_a, u, w, off = place(p)
        back = ((p // 2) % 2) == 0
        slot = jnp.where(back, (w + 1) % 4, (w + 3) % 4)
        to = jnp.where(back, (w + 3) % 4, (w + 1) % 4)
        return pltpu.make_async_remote_copy(
            src_ref=slab.at[p, core, slot],
            dst_ref=slab.at[p, core, slot],
            send_sem=send2.at[p, 2],
            recv_sem=recv2.at[p, 2],
            device_id=device(is_a, u, to),
            device_id_type=pl.DeviceIdType.MESH,
        )

    def third(p):
        return pltpu.make_async_remote_copy(
            src_ref=slab.at[p, core],
            dst_ref=slab.at[p, core],
            send_sem=send3.at[p],
            recv_sem=recv3.at[p],
            device_id={"vir": vir + 1 - 2 * core},
            device_id_type=pl.DeviceIdType.MESH,
        )

    def load(k):
        return pltpu.make_async_copy(vvvo_ref.at[k], vv.at[k], vsem.at[k])

    barrier = pltpu.get_barrier_semaphore()

    def greet(r, carry):
        pl.semaphore_signal(
            barrier, inc=1, device_id={"vir": (vir + r) % 32},
            device_id_type=pl.DeviceIdType.MESH)
        return carry

    lax.fori_loop(1, 32, greet, 0)
    for r in (1, 2, 3):
        pl.semaphore_signal(
            barrier, inc=1, device_id={"grp": (y + r) % 4},
            device_id_type=pl.DeviceIdType.MESH)

    for k in range(OW - 1, -1, -1):
        load(k).start()

    def fill(p, carry):
        q, j, k = pair_of(p)
        is_a, u, w, off = place(p)
        block = t2_ref[j, k]
        src[p, BLOCK - 12:, :] = jnp.zeros((ROWS - BLOCK + 12, V), jnp.bfloat16)
        src[p, :BLOCK, :] = block

        @pl.when(off == 0)
        def _():
            slab[p, core, w, BLOCK - 12:, :] = jnp.zeros((ROWS - BLOCK + 12, V), jnp.bfloat16)
            slab[p, core, w, :BLOCK, :] = block

        return carry

    lax.fori_loop(0, PAIRS, fill, 0)
    tile[...] = jnp.zeros_like(tile)
    tile[2:3, :] = jnp.sum(hit_ref[...], axis=0, keepdims=True)
    pl.semaphore_wait(barrier, 34)

    def start_first(p):
        copy, off = first(p)

        @pl.when(off != 0)
        def _():
            copy.start()

    for p in range(LEAD):
        start_first(p)

    def compute(p):
        q, j, k = pair_of(p)
        is_a, u, w, off = place(p)
        fresh = (p == 0) | (q == (k + 1) * (k + 2) // 2 - 1)

        @pl.when(fresh)
        def _():
            load(k).wait()

        cols = slab[p].reshape(2 * 4 * ROWS, V)
        wbuf[...] = lax.dot_general(vv[k], cols, NT_DIMS, preferred_element_type=jnp.float32)

        row = lax.broadcasted_iota(jnp.int32, (256, 1), 0)
        r_core = row // 128
        r_w = (row // ROWS) % 4
        r_in = row % ROWS
        source = (u + off) % 4
        owner = jnp.where(is_a, source * 8 + r_w * 2, r_w * 8 + source * 2) + r_core
        target = jnp.where(r_in < BLOCK, owner * BLOCK + r_in, -1)
        column = lax.broadcasted_iota(jnp.int32, (256, V), 1)
        select = (column == target).astype(jnp.float32).astype(jnp.bfloat16)
        holes = lax.dot_general(
            select, ih_ref[k, j], NT_DIMS, preferred_element_type=jnp.float32
        ).astype(jnp.bfloat16)
        variant = jnp.where(is_a, 0, 4) + source
        yc_row = yc_ref[pl.ds(variant, 1), :]
        lane = lax.broadcasted_iota(jnp.int32, (1, 128), 1)

        def one(i, carry):
            shift = occ_ref[i] + occ_ref[j] + occ_ref[k]
            yc = yc_row - shift
            for a in range(2):
                total = jnp.zeros((8, 256), jnp.float32)
                for c in range(V // CHUNK):
                    at = a * V + c * CHUNK
                    hole = lax.dot_general(
                        th_ref[i, at:at + CHUNK, :], holes, NT_DIMS,
                        preferred_element_type=jnp.float32)
                    amp = wbuf[at:at + CHUNK, :] + hole
                    base = xb_ref[at:at + CHUNK, :]
                    den = jnp.concatenate([base, base], axis=1) + yc
                    term = amp * amp / den
                    total = total + jnp.sum(term.reshape(CHUNK // 8, 8, 256), axis=0)
                line = jnp.sum(total, axis=0, keepdims=True)
                line = jnp.sum(line, axis=1, keepdims=True)
                tile[a:a + 1, :] = jnp.where(lane == q * OW + i, line, tile[a:a + 1, :])
            return carry

        lax.fori_loop(0, j + 1, one, 0)

    def step(s, carry):
        @pl.when(s + LEAD < PAIRS)
        def _():
            start_first(s + LEAD)

        @pl.when(s < PAIRS)
        def _():
            copy, off = first(s)

            @pl.when(off != 0)
            def _():
                copy.wait_recv()

            for turn in range(2):
                second(s, turn).start()

        @pl.when((s >= LAG2) & (s < PAIRS + LAG2))
        def _():
            for turn in range(2):
                second(s - LAG2, turn).wait_recv()
            relay(s - LAG2).start()

        @pl.when((s >= LAG3) & (s < PAIRS + LAG3))
        def _():
            relay(s - LAG3).wait_recv()
            third(s - LAG3).start()

        @pl.when(s >= LAG4)
        def _():
            third(s - LAG4).wait_recv()
            compute(s - LAG4)

        return carry

    lax.fori_loop(0, PAIRS + LAG4, step, 0)

    def drain(p, carry):
        copy, off = first(p)

        @pl.when(off != 0)
        def _():
            copy.wait_send()

        for turn in range(2):
            second(p, turn).wait_send()
        relay(p).wait_send()
        third(p).wait_send()
        return carry

    lax.fori_loop(0, PAIRS, drain, 0)

    def to_group(r):
        return pltpu.make_async_remote_copy(
            src_ref=tile,
            dst_ref=ybox.at[y],
            send_sem=ysend.at[r - 1],
            recv_sem=yrecv.at[r - 1],
            device_id={"grp": (y + r) % 4},
            device_id_type=pl.DeviceIdType.MESH,
        )

    for r in (1, 2, 3):
        to_group(r).start()
    ybox[y] = tile[...]
    for r in (1, 2, 3):
        to_group(r).wait_recv()
    whole = ybox[0] + ybox[1] + ybox[2] + ybox[3]
    mine = hit_ref[...] * (whole[0:1, :] + whole[1:2, :])
    part[...] = mine
    vbox[vir] = mine
    orb = jnp.sum(whole[2:3, :] * whole, axis=1, keepdims=True)
    orb_ref[...] = jnp.broadcast_to(orb, (8, 128))

    def to_plane(r, carry):
        pltpu.make_async_remote_copy(
            src_ref=part,
            dst_ref=vbox.at[vir],
            send_sem=psend,
            recv_sem=precv,
            device_id={"vir": (vir + r) % 32},
            device_id_type=pl.DeviceIdType.MESH,
        ).start()
        return carry

    lax.fori_loop(1, 32, to_plane, 0)
    for r in (1, 2, 3):
        to_group(r).wait_send()
    others = vbox.at[pl.ds(0, 31)]
    pltpu.make_async_copy(others, others, precv).wait()
    trip = jnp.sum(jnp.sum(vbox[...], axis=0), axis=1, keepdims=True)
    trip_ref[...] = jnp.broadcast_to(trip, (8, 128)) / 64
    pltpu.make_async_copy(others, others, psend).wait()


def pick_energy(a_pick, vir_energy):
    columns = jnp.arange(vir_energy.shape[0], dtype=jnp.int32)
    return jnp.sum(jnp.where(a_pick[:, None] == columns[None, :], vir_energy[None, :], 0.0), axis=1)


def tables(a_pick, vir_energy, t2hole):
    e_a = pick_energy(a_pick, vir_energy)
    base = (e_a[:, None] + vir_energy[None, :]).reshape(2 * V, 1)
    xb = jnp.broadcast_to(base, (2 * V, 128))
    split = vir_energy.reshape(4, 4, 2, BLOCK)
    split = jnp.pad(split, ((0, 0), (0, 0), (0, 0), (0, ROWS - BLOCK)), constant_values=1.0)
    by_x = jnp.transpose(split, (0, 2, 1, 3)).reshape(4, 256)
    by_z = jnp.transpose(split, (1, 2, 0, 3)).reshape(4, 256)
    yc = jnp.concatenate([by_x, by_z], axis=0)
    th = -jnp.transpose(t2hole, (0, 2, 3, 1)).reshape(OW, 2 * V, 60)
    return xb, yc, th


def partial_energies(t2pair, ints_vvvo, th, ints_hole, yc, xb, hit, occ_energy):
    vmem = pl.BlockSpec(memory_space=pltpu.VMEM)
    return pl.pallas_call(
        kernel,
        out_shape=[jax.ShapeDtypeStruct((8, 128), jnp.float32)] * 2,
        in_specs=[
            vmem, pl.BlockSpec(memory_space=pl.ANY), vmem, vmem, vmem, vmem, vmem,
            pl.BlockSpec(memory_space=pltpu.SMEM),
        ],
        out_specs=[vmem, vmem],
        scratch_shapes=[
            pltpu.VMEM((PAIRS, ROWS, V), jnp.bfloat16),
            pltpu.VMEM((PAIRS, 2, 4, ROWS, V), jnp.bfloat16),
            pltpu.VMEM((OW, 2 * V, V), jnp.bfloat16),
            pltpu.VMEM((2 * V, 256), jnp.float32),
            pltpu.SemaphoreType.DMA((PAIRS,)),
            pltpu.SemaphoreType.DMA((PAIRS,)),
            pltpu.SemaphoreType.DMA((PAIRS, 3)),
            pltpu.SemaphoreType.DMA((PAIRS, 3)),
            pltpu.SemaphoreType.DMA((PAIRS,)),
            pltpu.SemaphoreType.DMA((PAIRS,)),
            pltpu.SemaphoreType.DMA((OW,)),
            pltpu.VMEM((8, 128), jnp.float32),
            pltpu.VMEM((4, 8, 128), jnp.float32),
            pltpu.VMEM((8, 128), jnp.float32),
            pltpu.VMEM((32, 8, 128), jnp.float32),
            pltpu.SemaphoreType.DMA((3,)),
            pltpu.SemaphoreType.DMA((3,)),
            pltpu.SemaphoreType.DMA,
            pltpu.SemaphoreType.DMA,
        ],
        compiler_params=pltpu.CompilerParams(
            collective_id=0, has_side_effects=True, vmem_limit_bytes=60 * 1024 * 1024
        ),
    )(t2pair, ints_vvvo.reshape(OW, 2 * V, V), th, ints_hole, yc, xb, hit, occ_energy)


def shards(
    triplets, counts, weights, a_pick, occ_energy, vir_energy, ints_vvvo, t2pair, t2hole, ints_hole
):
    slots = triplets.shape[0]
    xb, yc, th = tables(a_pick, vir_energy, t2hole)
    code = (triplets[:, 2] * (triplets[:, 2] + 1) // 2 + triplets[:, 1]) * OW + triplets[:, 0]
    live = jnp.arange(slots, dtype=jnp.int32) < counts[0]
    factor = jnp.where(live, -weights.astype(jnp.float32) / (V * V), 0.0)
    lanes = jnp.arange(128, dtype=jnp.int32)
    hit = jnp.where(code[:, None] == lanes[None, :], factor[:, None], 0.0)
    hit = jnp.pad(hit, ((0, 8 - slots), (0, 0)))
    trip, orbital = partial_energies(t2pair, ints_vvvo, th, ints_hole, yc, xb, hit, occ_energy)
    return (trip[:slots, 0], orbital[:2, 0])


def solution(mesh):
    placed = (
        P("grp", None),
        P("grp"),
        P("grp"),
        P("vir"),
        P(),
        P(),
        P(None, "vir", None, None),
        P(None, None, "vir", None),
        P(None, None, "vir", None),
        P(),
    )
    return jax.shard_map(
        shards, mesh=mesh, in_specs=placed, out_specs=(P("grp"), P("vir")), check_vma=False
    )
```

```python
import jax
import jax.numpy as jnp
from jax import lax
from jax.experimental import pallas as pl
from jax.experimental.pallas import tpu as pltpu
from jax.sharding import PartitionSpec as P

V = 896
BLOCK = 28
ROWS = 32
PAIRS = 15
OW = 5
LEAD = 4
LAG2 = 3
LAG3 = 6
LAG4 = 8
CHUNK = 224
NT_DIMS = (((1,), (1,)), ((), ()))


def pair_of(step):
    q = PAIRS - 1 - step
    k = (
        (q >= 1).astype(jnp.int32)
        + (q >= 3).astype(jnp.int32)
        + (q >= 6).astype(jnp.int32)
        + (q >= 10).astype(jnp.int32)
    )
    return q, q - k * (k + 1) // 2, k


def kernel(
    t2_ref, vvvo_ref, hole_hbm, ih_hbm, vir_ref, yc_ref, hit_ref, occ_ref, vsm_ref, pick_ref,
    trip_ref, orb_ref, src, slab, vv, wbuf, th_ref, hole_ref, ih_ref, xb_ref, isem, send1, recv1, send2, recv2, send3, recv3, vsem,
    tile, ybox, part, vbox, ysend, yrecv, psend, precv,
):
    y = lax.axis_index("grp")
    vir = lax.axis_index("vir")
    core = vir % 2
    x = vir // 8
    z = (vir // 2) % 4

    def place(p):
        is_a = (p % 2) == 0
        u = jnp.where(is_a, x, z)
        w = jnp.where(is_a, z, x)
        off = (y + p // 2) % 4
        return is_a, u, w, off

    def device(is_a, u, w):
        return {"vir": jnp.where(is_a, u * 8 + w * 2, w * 8 + u * 2) + core}

    def first(p):
        is_a, u, w, off = place(p)
        return pltpu.make_async_remote_copy(
            src_ref=src.at[p],
            dst_ref=slab.at[p, core, w, :, pl.ds(0, V)],
            send_sem=send1.at[p],
            recv_sem=recv1.at[p],
            device_id=device(is_a, (u + 4 - off) % 4, w),
            device_id_type=pl.DeviceIdType.MESH,
        ), off

    def second(p, turn):
        is_a, u, w, off = place(p)
        shift = (1, 3)[turn]
        return pltpu.make_async_remote_copy(
            src_ref=slab.at[p, core, w, :, pl.ds(0, V)],
            dst_ref=slab.at[p, core, w, :, pl.ds(0, V)],
            send_sem=send2.at[p, turn],
            recv_sem=recv2.at[p, turn],
            device_id=device(is_a, u, (w + shift) % 4),
            device_id_type=pl.DeviceIdType.MESH,
        )

    def relay(p):
        is_a, u, w, off = place(p)
        back = ((p // 2) % 2) == 0
        slot = jnp.where(back, (w + 1) % 4, (w + 3) % 4)
        to = jnp.where(back, (w + 3) % 4, (w + 1) % 4)
        return pltpu.make_async_remote_copy(
            src_ref=slab.at[p, core, slot, :, pl.ds(0, V)],
            dst_ref=slab.at[p, core, slot, :, pl.ds(0, V)],
            send_sem=send2.at[p, 2],
            recv_sem=recv2.at[p, 2],
            device_id=device(is_a, u, to),
            device_id_type=pl.DeviceIdType.MESH,
        )

    def third(p):
        return pltpu.make_async_remote_copy(
            src_ref=slab.at[p, core, :, :, pl.ds(0, V)],
            dst_ref=slab.at[p, core, :, :, pl.ds(0, V)],
            send_sem=send3.at[p],
            recv_sem=recv3.at[p],
            device_id={"vir": vir + 1 - 2 * core},
            device_id_type=pl.DeviceIdType.MESH,
        )

    def load(k):
        return pltpu.make_async_copy(vvvo_ref.at[k], vv.at[k, :, pl.ds(0, V)], vsem.at[k])

    barrier = pltpu.get_barrier_semaphore()

    def greet(r, carry):
        pl.semaphore_signal(
            barrier, inc=1, device_id={"vir": (vir + r) % 32},
            device_id_type=pl.DeviceIdType.MESH)
        return carry

    lax.fori_loop(1, 32, greet, 0)
    for r in (1, 2, 3):
        pl.semaphore_signal(
            barrier, inc=1, device_id={"grp": (y + r) % 4},
            device_id_type=pl.DeviceIdType.MESH)

    holes_in = pltpu.make_async_copy(hole_hbm, hole_ref, isem.at[0])
    ints_in = pltpu.make_async_copy(ih_hbm, ih_ref, isem.at[1])
    holes_in.start()
    load(OW - 1).start()
    ints_in.start()
    for k in range(OW - 2, -1, -1):
        load(k).start()

    def fill(p, carry):
        q, j, k = pair_of(p)
        is_a, u, w, off = place(p)
        block = t2_ref[j, k]
        src[p, BLOCK - 12:, :] = jnp.zeros((ROWS - BLOCK + 12, V), jnp.bfloat16)
        src[p, :BLOCK, :] = block

        @pl.when(off == 0)
        def _():
            slab[p, core, w, BLOCK - 12:, :V] = jnp.zeros((ROWS - BLOCK + 12, V), jnp.bfloat16)
            slab[p, core, w, :BLOCK, :V] = block

        return carry

    lax.fori_loop(0, PAIRS, fill, 0)
    for a in range(2):
        e_a = vsm_ref[pick_ref[a]]
        for c in range(V // 128):
            lines = jnp.broadcast_to(vir_ref[:, c * 128:(c + 1) * 128], (128, 128))
            xb_ref[a * V + c * 128:a * V + (c + 1) * 128, :] = lines.T + e_a
    tile[...] = jnp.zeros_like(tile)
    tile[2:3, :] = jnp.sum(hit_ref[...], axis=0, keepdims=True)
    pl.semaphore_wait(barrier, 34)

    def start_first(p):
        copy, off = first(p)

        @pl.when(off != 0)
        def _():
            copy.start()

    for p in range(LEAD):
        start_first(p)

    def turn_holes(i):
        for c in range(2 * V // 128):
            at = c * 128
            base = hole_ref[0, :, at:at + 128].astype(jnp.float32)
            this = hole_ref[i, :, at:at + 128].astype(jnp.float32)
            both = jnp.concatenate([base, -this], axis=0)
            th_ref[i, at:at + 128, :] = both.T.astype(jnp.bfloat16)

    def base_holes():
        for c in range(2 * V // 128):
            at = c * 128
            base = hole_ref[0, :, at:at + 128].astype(jnp.float32)
            both = jnp.concatenate([-base, jnp.zeros_like(base)], axis=0)
            turned = both.T.astype(jnp.bfloat16)
            for k in range(OW):
                vv[k, at:at + 128, V:] = turned

    def compute(p):
        q, j, k = pair_of(p)
        is_a, u, w, off = place(p)
        fresh = (p == 0) | (q == (k + 1) * (k + 2) // 2 - 1)

        @pl.when(fresh)
        def _():
            load(k).wait()

        row = lax.broadcasted_iota(jnp.int32, (256, 1), 0)
        r_core = row // 128
        r_w = (row // ROWS) % 4
        r_in = row % ROWS
        source = (u + off) % 4
        owner = jnp.where(is_a, source * 8 + r_w * 2, r_w * 8 + source * 2) + r_core
        target = jnp.where(r_in < BLOCK, owner * BLOCK + r_in, -1)
        column = lax.broadcasted_iota(jnp.int32, (256, V), 1)
        select = (column == target).astype(jnp.float32).astype(jnp.bfloat16)
        holes = lax.dot_general(
            select, ih_ref[k, j], NT_DIMS, preferred_element_type=jnp.float32
        )
        blank = jnp.zeros((256, 4), jnp.float32)
        holes = jnp.concatenate([holes, blank, holes, blank], axis=1).astype(jnp.bfloat16)
        slab[p, :, :, :, V:] = holes.reshape(2, 4, ROWS, 128)
        cols = slab[p].reshape(2 * 4 * ROWS, 1024)
        wbuf[...] = lax.dot_general(vv[k], cols, NT_DIMS, preferred_element_type=jnp.float32)
        variant = jnp.where(is_a, 0, 4) + source
        yc_row = yc_ref[pl.ds(variant, 1), :]
        lane = lax.broadcasted_iota(jnp.int32, (1, 128), 1)

        def terms(amp, at, yc):
            base = xb_ref[at:at + CHUNK, :]
            den = jnp.concatenate([base, base], axis=1) + yc
            term = amp * amp / den
            return jnp.sum(term.reshape(CHUNK // 8, 8, 256), axis=0)

        def put(total, i, a):
            line = jnp.sum(total, axis=0, keepdims=True)
            line = jnp.sum(line, axis=1, keepdims=True)
            tile[a:a + 1, :] = jnp.where(lane == q * OW + i, line, tile[a:a + 1, :])

        yc = yc_row - (occ_ref[0] + occ_ref[j] + occ_ref[k])
        for a in range(2):
            total = jnp.zeros((8, 256), jnp.float32)
            for c in range(V // CHUNK):
                at = a * V + c * CHUNK
                total = total + terms(wbuf[at:at + CHUNK, :], at, yc)
            put(total, 0, a)

        def one(i, carry):
            yc = yc_row - (occ_ref[i] + occ_ref[j] + occ_ref[k])
            for a in range(2):
                total = jnp.zeros((8, 256), jnp.float32)
                for c in range(V // CHUNK):
                    at = a * V + c * CHUNK
                    hole = lax.dot_general(
                        th_ref[i, at:at + CHUNK, :], holes, NT_DIMS,
                        preferred_element_type=jnp.float32)
                    total = total + terms(wbuf[at:at + CHUNK, :] + hole, at, yc)
                put(total, i, a)
            return carry

        lax.fori_loop(1, j + 1, one, 0)

    def step(s, carry):
        @pl.when(s + LEAD < PAIRS)
        def _():
            start_first(s + LEAD)

        @pl.when(s < PAIRS)
        def _():
            copy, off = first(s)

            @pl.when(off != 0)
            def _():
                copy.wait_recv()

            for turn in range(2):
                second(s, turn).start()

        @pl.when((s >= LAG2) & (s < PAIRS + LAG2))
        def _():
            for turn in range(2):
                second(s - LAG2, turn).wait_recv()
            relay(s - LAG2).start()

        @pl.when((s >= LAG3) & (s < PAIRS + LAG3))
        def _():
            relay(s - LAG3).wait_recv()
            third(s - LAG3).start()

        @pl.when(s == 1)
        def _():
            holes_in.wait()
            base_holes()

        @pl.when((s >= 2) & (s < OW + 1))
        def _():
            turn_holes(s - 1)

        @pl.when(s == OW + 1)
        def _():
            ints_in.wait()

        @pl.when(s >= LAG4)
        def _():
            third(s - LAG4).wait_recv()
            compute(s - LAG4)

        return carry

    lax.fori_loop(0, PAIRS + LAG4, step, 0)

    def drain(p, carry):
        copy, off = first(p)

        @pl.when(off != 0)
        def _():
            copy.wait_send()

        for turn in range(2):
            second(p, turn).wait_send()
        relay(p).wait_send()
        third(p).wait_send()
        return carry

    lax.fori_loop(0, PAIRS, drain, 0)

    def to_group(r):
        return pltpu.make_async_remote_copy(
            src_ref=tile,
            dst_ref=ybox.at[y],
            send_sem=ysend.at[r - 1],
            recv_sem=yrecv.at[r - 1],
            device_id={"grp": (y + r) % 4},
            device_id_type=pl.DeviceIdType.MESH,
        )

    for r in (1, 2, 3):
        to_group(r).start()
    ybox[y] = tile[...]
    for r in (1, 2, 3):
        to_group(r).wait_recv()
    whole = ybox[0] + ybox[1] + ybox[2] + ybox[3]
    mine = hit_ref[...] * (whole[0:1, :] + whole[1:2, :])
    part[...] = mine
    vbox[vir] = mine
    orb = jnp.sum(whole[2:3, :] * whole, axis=1, keepdims=True)
    orb_ref[...] = jnp.broadcast_to(orb, (8, 128))

    def to_plane(r, carry):
        pltpu.make_async_remote_copy(
            src_ref=part,
            dst_ref=vbox.at[vir],
            send_sem=psend,
            recv_sem=precv,
            device_id={"vir": (vir + r) % 32},
            device_id_type=pl.DeviceIdType.MESH,
        ).start()
        return carry

    lax.fori_loop(1, 32, to_plane, 0)
    for r in (1, 2, 3):
        to_group(r).wait_send()
    others = vbox.at[pl.ds(0, 31)]
    pltpu.make_async_copy(others, others, precv).wait()
    trip = jnp.sum(jnp.sum(vbox[...], axis=0), axis=1, keepdims=True)
    trip_ref[...] = jnp.broadcast_to(trip, (8, 128)) / 64
    pltpu.make_async_copy(others, others, psend).wait()


def tables(vir_energy, t2hole):
    split = vir_energy.reshape(4, 4, 2, BLOCK)
    split = jnp.pad(split, ((0, 0), (0, 0), (0, 0), (0, ROWS - BLOCK)), constant_values=1.0)
    by_x = jnp.transpose(split, (0, 2, 1, 3)).reshape(4, 256)
    by_z = jnp.transpose(split, (1, 2, 0, 3)).reshape(4, 256)
    yc = jnp.concatenate([by_x, by_z], axis=0)
    holes = jnp.pad(t2hole.reshape(OW, 60, 2 * V), ((0, 0), (0, 4), (0, 0)))
    return yc, holes


def partial_energies(t2pair, ints_vvvo, holes, ints_hole, vir_energy, yc, hit, occ_energy, a_pick):
    vmem = pl.BlockSpec(memory_space=pltpu.VMEM)
    smem = pl.BlockSpec(memory_space=pltpu.SMEM)
    hbm = pl.BlockSpec(memory_space=pl.ANY)
    return pl.pallas_call(
        kernel,
        out_shape=[jax.ShapeDtypeStruct((8, 128), jnp.float32)] * 2,
        in_specs=[
            vmem, hbm, hbm, hbm, vmem, vmem, vmem, smem, smem, smem,
        ],
        out_specs=[vmem, vmem],
        scratch_shapes=[
            pltpu.VMEM((PAIRS, ROWS, V), jnp.bfloat16),
            pltpu.VMEM((PAIRS, 2, 4, ROWS, 1024), jnp.bfloat16),
            pltpu.VMEM((OW, 2 * V, 1024), jnp.bfloat16),
            pltpu.VMEM((2 * V, 256), jnp.float32),
            pltpu.VMEM((OW, 2 * V, 128), jnp.bfloat16),
            pltpu.VMEM((OW, 64, 2 * V), jnp.bfloat16),
            pltpu.VMEM((OW, OW, 60, V), jnp.bfloat16),
            pltpu.VMEM((2 * V, 128), jnp.float32),
            pltpu.SemaphoreType.DMA((2,)),
            pltpu.SemaphoreType.DMA((PAIRS,)),
            pltpu.SemaphoreType.DMA((PAIRS,)),
            pltpu.SemaphoreType.DMA((PAIRS, 3)),
            pltpu.SemaphoreType.DMA((PAIRS, 3)),
            pltpu.SemaphoreType.DMA((PAIRS,)),
            pltpu.SemaphoreType.DMA((PAIRS,)),
            pltpu.SemaphoreType.DMA((OW,)),
            pltpu.VMEM((8, 128), jnp.float32),
            pltpu.VMEM((4, 8, 128), jnp.float32),
            pltpu.VMEM((8, 128), jnp.float32),
            pltpu.VMEM((32, 8, 128), jnp.float32),
            pltpu.SemaphoreType.DMA((3,)),
            pltpu.SemaphoreType.DMA((3,)),
            pltpu.SemaphoreType.DMA,
            pltpu.SemaphoreType.DMA,
        ],
        compiler_params=pltpu.CompilerParams(
            collective_id=0, has_side_effects=True, vmem_limit_bytes=60 * 1024 * 1024
        ),
    )(
        t2pair, ints_vvvo.reshape(OW, 2 * V, V), holes, ints_hole,
        vir_energy.reshape(1, V), yc, hit, occ_energy, vir_energy, a_pick,
    )


def shards(
    triplets, counts, weights, a_pick, occ_energy, vir_energy, ints_vvvo, t2pair, t2hole, ints_hole
):
    slots = triplets.shape[0]
    yc, holes = tables(vir_energy, t2hole)
    code = (triplets[:, 2] * (triplets[:, 2] + 1) // 2 + triplets[:, 1]) * OW + triplets[:, 0]
    live = jnp.arange(slots, dtype=jnp.int32) < counts[0]
    factor = jnp.where(live, -weights.astype(jnp.float32) / (V * V), 0.0)
    lanes = jnp.arange(128, dtype=jnp.int32)
    hit = jnp.where(code[:, None] == lanes[None, :], factor[:, None], 0.0)
    hit = jnp.pad(hit, ((0, 8 - slots), (0, 0)))
    trip, orbital = partial_energies(
        t2pair, ints_vvvo, holes, ints_hole, vir_energy, yc, hit, occ_energy, a_pick
    )
    return (trip[:slots, 0], orbital[:2, 0])


def solution(mesh):
    placed = (
        P("grp", None),
        P("grp"),
        P("grp"),
        P("vir"),
        P(),
        P(),
        P(None, "vir", None, None),
        P(None, None, "vir", None),
        P(None, None, "vir", None),
        P(),
    )
    return jax.shard_map(
        shards, mesh=mesh, in_specs=placed, out_specs=(P("grp"), P("vir")), check_vma=False
    )
```

```python
import jax
import jax.numpy as jnp
from jax import lax
from jax.experimental import pallas as pl
from jax.experimental.pallas import tpu as pltpu
from jax.sharding import PartitionSpec as P

V = 896
BLOCK = 28
ROWS = 32
PAIRS = 15
OW = 5
LEAD = 4
LAG2 = 3
LAG3 = 3
LAG4 = 5
EARLY = 15
CHUNK = 224
NT_DIMS = (((1,), (1,)), ((), ()))


def pair_of(step):
    q = PAIRS - 1 - step
    k = (
        (q >= 1).astype(jnp.int32)
        + (q >= 3).astype(jnp.int32)
        + (q >= 6).astype(jnp.int32)
        + (q >= 10).astype(jnp.int32)
    )
    return q, q - k * (k + 1) // 2, k


def kernel(
    t2_ref, vvvo_ref, hole_hbm, ih_hbm, vir_ref, yc_ref, hit_ref, occ_ref, vsm_ref, pick_ref,
    trip_ref, orb_ref, src, slab, vv, wbuf, th_ref, hole_ref, ih_ref, xb_ref, isem, send1, recv1, send2, recv2, send3, recv3, vsem,
    tile, ybox, part, vbox, ysend, yrecv, psend, precv,
):
    y = lax.axis_index("grp")
    vir = lax.axis_index("vir")
    core = vir % 2
    x = vir // 8
    z = (vir // 2) % 4

    def place(p):
        is_a = (p % 2) == 0
        u = jnp.where(is_a, x, z)
        w = jnp.where(is_a, z, x)
        off = (y + p // 2) % 4
        return is_a, u, w, off

    def device(is_a, u, w):
        return {"vir": jnp.where(is_a, u * 8 + w * 2, w * 8 + u * 2) + core}

    def first(p):
        is_a, u, w, off = place(p)
        return pltpu.make_async_remote_copy(
            src_ref=src.at[p],
            dst_ref=slab.at[p, core, w, :, pl.ds(0, V)],
            send_sem=send1.at[p],
            recv_sem=recv1.at[p],
            device_id=device(is_a, (u + 4 - off) % 4, w),
            device_id_type=pl.DeviceIdType.MESH,
        ), off

    def second(p, turn):
        is_a, u, w, off = place(p)
        shift = (1, 3, 2)[turn]
        return pltpu.make_async_remote_copy(
            src_ref=slab.at[p, core, w, :, pl.ds(0, V)],
            dst_ref=slab.at[p, core, w, :, pl.ds(0, V)],
            send_sem=send2.at[p, turn],
            recv_sem=recv2.at[p, turn],
            device_id=device(is_a, u, (w + shift) % 4),
            device_id_type=pl.DeviceIdType.MESH,
        )

    def relay(p):
        is_a, u, w, off = place(p)
        back = ((p // 2) % 2) == 0
        slot = jnp.where(back, (w + 1) % 4, (w + 3) % 4)
        to = jnp.where(back, (w + 3) % 4, (w + 1) % 4)
        return pltpu.make_async_remote_copy(
            src_ref=slab.at[p, core, slot, :, pl.ds(0, V)],
            dst_ref=slab.at[p, core, slot, :, pl.ds(0, V)],
            send_sem=send2.at[p, 2],
            recv_sem=recv2.at[p, 2],
            device_id=device(is_a, u, to),
            device_id_type=pl.DeviceIdType.MESH,
        )

    def third(p):
        return pltpu.make_async_remote_copy(
            src_ref=slab.at[p, core, :, :, pl.ds(0, V)],
            dst_ref=slab.at[p, core, :, :, pl.ds(0, V)],
            send_sem=send3.at[p],
            recv_sem=recv3.at[p],
            device_id={"vir": vir + 1 - 2 * core},
            device_id_type=pl.DeviceIdType.MESH,
        )

    def load(k):
        return pltpu.make_async_copy(vvvo_ref.at[k], vv.at[k, :, pl.ds(0, V)], vsem.at[k])

    barrier = pltpu.get_barrier_semaphore()

    def greet(r, carry):
        pl.semaphore_signal(
            barrier, inc=1, device_id={"vir": (vir + r) % 32},
            device_id_type=pl.DeviceIdType.MESH)
        return carry

    lax.fori_loop(1, 32, greet, 0)
    for r in (1, 2, 3):
        pl.semaphore_signal(
            barrier, inc=1, device_id={"grp": (y + r) % 4},
            device_id_type=pl.DeviceIdType.MESH)

    holes_in = pltpu.make_async_copy(hole_hbm, hole_ref, isem.at[0])
    ints_in = pltpu.make_async_copy(ih_hbm, ih_ref, isem.at[1])
    holes_in.start()
    ints_in.start()
    load(OW - 1).start()
    for k in range(OW - 2, -1, -1):
        load(k).start()

    def fill(p, carry):
        q, j, k = pair_of(p)
        is_a, u, w, off = place(p)
        block = t2_ref[j, k]
        src[p, BLOCK - 12:, :] = jnp.zeros((ROWS - BLOCK + 12, V), jnp.bfloat16)
        src[p, :BLOCK, :] = block

        @pl.when(off == 0)
        def _():
            slab[p, core, w, BLOCK - 12:, :V] = jnp.zeros((ROWS - BLOCK + 12, V), jnp.bfloat16)
            slab[p, core, w, :BLOCK, :V] = block

        return carry

    lax.fori_loop(0, PAIRS, fill, 0)
    for a in range(2):
        e_a = vsm_ref[pick_ref[a]]
        for c in range(V // 128):
            lines = jnp.broadcast_to(vir_ref[:, c * 128:(c + 1) * 128], (128, 128))
            xb_ref[a * V + c * 128:a * V + (c + 1) * 128, :] = lines.T + e_a
    tile[...] = jnp.zeros_like(tile)
    tile[2:3, :] = jnp.sum(hit_ref[...], axis=0, keepdims=True)
    pl.semaphore_wait(barrier, 34)

    def start_first(p):
        copy, off = first(p)

        @pl.when(off != 0)
        def _():
            copy.start()

    for p in range(LEAD):
        start_first(p)

    def read_holes(i, at):
        some = hole_ref[i, :, at:at + 128].astype(jnp.float32)
        return jnp.concatenate([some, jnp.zeros((4, 128), jnp.float32)], axis=0)

    def turn_holes(i):
        for c in range(2 * V // 128):
            at = c * 128
            base = read_holes(0, at)
            this = read_holes(i, at)
            both = jnp.concatenate([base, -this], axis=0)
            th_ref[i, at:at + 128, :] = both.T.astype(jnp.bfloat16)

    def base_holes():
        for c in range(2 * V // 128):
            at = c * 128
            base = read_holes(0, at)
            both = jnp.concatenate([-base, jnp.zeros_like(base)], axis=0)
            turned = both.T.astype(jnp.bfloat16)
            for k in range(OW):
                vv[k, at:at + 128, V:] = turned

    def prepare(p, carry):
        q, j, k = pair_of(p)
        is_a, u, w, off = place(p)
        row = lax.broadcasted_iota(jnp.int32, (256, 1), 0)
        r_core = row // 128
        r_w = (row // ROWS) % 4
        r_in = row % ROWS
        source = (u + off) % 4
        owner = jnp.where(is_a, source * 8 + r_w * 2, r_w * 8 + source * 2) + r_core
        target = jnp.where(r_in < BLOCK, owner * BLOCK + r_in, -1)
        column = lax.broadcasted_iota(jnp.int32, (256, V), 1)
        select = (column == target).astype(jnp.float32).astype(jnp.bfloat16)
        holes = lax.dot_general(
            select, ih_ref[k, j], NT_DIMS, preferred_element_type=jnp.float32
        )
        blank = jnp.zeros((256, 4), jnp.float32)
        holes = jnp.concatenate([holes, blank, holes, blank], axis=1).astype(jnp.bfloat16)
        slab[p, :, :, :, V:] = holes.reshape(2, 4, ROWS, 128)
        return carry

    def compute(p):
        q, j, k = pair_of(p)
        is_a, u, w, off = place(p)
        fresh = (p == 0) | (q == (k + 1) * (k + 2) // 2 - 1)

        @pl.when(fresh)
        def _():
            load(k).wait()

        source = (u + off) % 4
        cols = slab[p].reshape(2 * 4 * ROWS, 1024)
        wbuf[...] = lax.dot_general(vv[k], cols, NT_DIMS, preferred_element_type=jnp.float32)
        holes = slab[p, :, :, :, V:].reshape(256, 128)
        variant = jnp.where(is_a, 0, 4) + source
        yc_row = yc_ref[pl.ds(variant, 1), :]
        lane = lax.broadcasted_iota(jnp.int32, (1, 128), 1)

        def terms(amp, at, yc):
            base = xb_ref[at:at + CHUNK, :]
            den = jnp.concatenate([base, base], axis=1) + yc
            term = amp * amp / den
            return jnp.sum(term.reshape(CHUNK // 8, 8, 256), axis=0)

        def put(total, i, a):
            line = jnp.sum(total, axis=0, keepdims=True)
            line = jnp.sum(line, axis=1, keepdims=True)
            tile[a:a + 1, :] = jnp.where(lane == q * OW + i, line, tile[a:a + 1, :])

        yc = yc_row - (occ_ref[0] + occ_ref[j] + occ_ref[k])
        for a in range(2):
            total = jnp.zeros((8, 256), jnp.float32)
            for c in range(V // CHUNK):
                at = a * V + c * CHUNK
                total = total + terms(wbuf[at:at + CHUNK, :], at, yc)
            put(total, 0, a)

        def one(i, carry):
            yc = yc_row - (occ_ref[i] + occ_ref[j] + occ_ref[k])
            for a in range(2):
                total = jnp.zeros((8, 256), jnp.float32)
                for c in range(V // CHUNK):
                    at = a * V + c * CHUNK
                    hole = lax.dot_general(
                        th_ref[i, at:at + CHUNK, :], holes, NT_DIMS,
                        preferred_element_type=jnp.float32)
                    total = total + terms(wbuf[at:at + CHUNK, :] + hole, at, yc)
                put(total, i, a)
            return carry

        lax.fori_loop(1, j + 1, one, 0)

    def step(s, carry):
        @pl.when(s + LEAD < PAIRS)
        def _():
            start_first(s + LEAD)

        @pl.when(s < PAIRS)
        def _():
            copy, off = first(s)

            @pl.when(off != 0)
            def _():
                copy.wait_recv()

            for turn in range(2):
                second(s, turn).start()

            @pl.when(s < EARLY)
            def _():
                second(s, 2).start()

        @pl.when((s >= LAG2) & (s < PAIRS + LAG2))
        def _():
            for turn in range(2):
                second(s - LAG2, turn).wait_recv()

            @pl.when(s - LAG2 >= EARLY)
            def _():
                relay(s - LAG2).start()

        @pl.when((s >= LAG3) & (s < PAIRS + LAG3))
        def _():
            relay(s - LAG3).wait_recv()
            third(s - LAG3).start()

        @pl.when(s == 0)
        def _():
            ints_in.wait()
            holes_in.wait()
            base_holes()

        @pl.when((s >= 1) & (s < OW))
        def _():
            turn_holes(s)

        @pl.when(s < 5)
        def _():
            lax.fori_loop(3 * s, 3 * s + 3, prepare, 0)

        @pl.when(s >= LAG4)
        def _():
            third(s - LAG4).wait_recv()
            compute(s - LAG4)

        return carry

    lax.fori_loop(0, PAIRS + LAG4, step, 0)

    def drain(p, carry):
        copy, off = first(p)

        @pl.when(off != 0)
        def _():
            copy.wait_send()

        return carry

    def drain_rest(p, carry):
        for turn in range(2):
            second(p, turn).wait_send()
        relay(p).wait_send()
        third(p).wait_send()
        return carry

    lax.fori_loop(0, PAIRS, drain, 0)

    def to_group(r):
        return pltpu.make_async_remote_copy(
            src_ref=tile,
            dst_ref=ybox.at[y],
            send_sem=ysend.at[r - 1],
            recv_sem=yrecv.at[r - 1],
            device_id={"grp": (y + r) % 4},
            device_id_type=pl.DeviceIdType.MESH,
        )

    for r in (1, 2, 3):
        to_group(r).start()
    ybox[y] = tile[...]
    lax.fori_loop(0, PAIRS, drain_rest, 0)
    for r in (1, 2, 3):
        to_group(r).wait_recv()
    whole = ybox[0] + ybox[1] + ybox[2] + ybox[3]
    mine = hit_ref[...] * (whole[0:1, :] + whole[1:2, :])
    part[...] = mine
    vbox[vir] = mine
    orb = jnp.sum(whole[2:3, :] * whole, axis=1, keepdims=True)
    orb_ref[...] = jnp.broadcast_to(orb, (8, 128))

    def to_plane(r, carry):
        pltpu.make_async_remote_copy(
            src_ref=part,
            dst_ref=vbox.at[vir],
            send_sem=psend,
            recv_sem=precv,
            device_id={"vir": (vir + r) % 32},
            device_id_type=pl.DeviceIdType.MESH,
        ).start()
        return carry

    lax.fori_loop(1, 32, to_plane, 0)
    for r in (1, 2, 3):
        to_group(r).wait_send()
    others = vbox.at[pl.ds(0, 31)]
    pltpu.make_async_copy(others, others, precv).wait()
    trip = jnp.sum(jnp.sum(vbox[...], axis=0), axis=1, keepdims=True)
    trip_ref[...] = jnp.broadcast_to(trip, (8, 128)) / 64
    pltpu.make_async_copy(others, others, psend).wait()


def tables(vir_energy, t2hole):
    split = vir_energy.reshape(4, 4, 2, BLOCK)
    split = jnp.pad(split, ((0, 0), (0, 0), (0, 0), (0, ROWS - BLOCK)), constant_values=1.0)
    by_x = jnp.transpose(split, (0, 2, 1, 3)).reshape(4, 256)
    by_z = jnp.transpose(split, (1, 2, 0, 3)).reshape(4, 256)
    yc = jnp.concatenate([by_x, by_z], axis=0)
    holes = t2hole.reshape(OW, 60, 2 * V)
    return yc, holes


def partial_energies(t2pair, ints_vvvo, holes, ints_hole, vir_energy, yc, hit, occ_energy, a_pick):
    vmem = pl.BlockSpec(memory_space=pltpu.VMEM)
    smem = pl.BlockSpec(memory_space=pltpu.SMEM)
    hbm = pl.BlockSpec(memory_space=pl.ANY)
    return pl.pallas_call(
        kernel,
        out_shape=[jax.ShapeDtypeStruct((8, 128), jnp.float32)] * 2,
        in_specs=[
            vmem, hbm, hbm, hbm, vmem, vmem, vmem, smem, smem, smem,
        ],
        out_specs=[vmem, vmem],
        scratch_shapes=[
            pltpu.VMEM((PAIRS, ROWS, V), jnp.bfloat16),
            pltpu.VMEM((PAIRS, 2, 4, ROWS, 1024), jnp.bfloat16),
            pltpu.VMEM((OW, 2 * V, 1024), jnp.bfloat16),
            pltpu.VMEM((2 * V, 256), jnp.float32),
            pltpu.VMEM((OW, 2 * V, 128), jnp.bfloat16),
            pltpu.VMEM((OW, 60, 2 * V), jnp.bfloat16),
            pltpu.VMEM((OW, OW, 60, V), jnp.bfloat16),
            pltpu.VMEM((2 * V, 128), jnp.float32),
            pltpu.SemaphoreType.DMA((2,)),
            pltpu.SemaphoreType.DMA((PAIRS,)),
            pltpu.SemaphoreType.DMA((PAIRS,)),
            pltpu.SemaphoreType.DMA((PAIRS, 3)),
            pltpu.SemaphoreType.DMA((PAIRS, 3)),
            pltpu.SemaphoreType.DMA((PAIRS,)),
            pltpu.SemaphoreType.DMA((PAIRS,)),
            pltpu.SemaphoreType.DMA((OW,)),
            pltpu.VMEM((8, 128), jnp.float32),
            pltpu.VMEM((4, 8, 128), jnp.float32),
            pltpu.VMEM((8, 128), jnp.float32),
            pltpu.VMEM((32, 8, 128), jnp.float32),
            pltpu.SemaphoreType.DMA((3,)),
            pltpu.SemaphoreType.DMA((3,)),
            pltpu.SemaphoreType.DMA,
            pltpu.SemaphoreType.DMA,
        ],
        compiler_params=pltpu.CompilerParams(
            collective_id=0, has_side_effects=True, vmem_limit_bytes=60 * 1024 * 1024
        ),
    )(
        t2pair, ints_vvvo.reshape(OW, 2 * V, V), holes, ints_hole,
        vir_energy.reshape(1, V), yc, hit, occ_energy, vir_energy, a_pick,
    )


def shards(
    triplets, counts, weights, a_pick, occ_energy, vir_energy, ints_vvvo, t2pair, t2hole, ints_hole
):
    slots = triplets.shape[0]
    yc, holes = tables(vir_energy, t2hole)
    code = (triplets[:, 2] * (triplets[:, 2] + 1) // 2 + triplets[:, 1]) * OW + triplets[:, 0]
    live = jnp.arange(slots, dtype=jnp.int32) < counts[0]
    factor = jnp.where(live, -weights.astype(jnp.float32) / (V * V), 0.0)
    lanes = jnp.arange(128, dtype=jnp.int32)
    hit = jnp.where(code[:, None] == lanes[None, :], factor[:, None], 0.0)
    hit = jnp.pad(hit, ((0, 8 - slots), (0, 0)))
    trip, orbital = partial_energies(
        t2pair, ints_vvvo, holes, ints_hole, vir_energy, yc, hit, occ_energy, a_pick
    )
    return (trip[:slots, 0], orbital[:2, 0])


def solution(mesh):
    placed = (
        P("grp", None),
        P("grp"),
        P("grp"),
        P("vir"),
        P(),
        P(),
        P(None, "vir", None, None),
        P(None, None, "vir", None),
        P(None, None, "vir", None),
        P(),
    )
    return jax.shard_map(
        shards, mesh=mesh, in_specs=placed, out_specs=(P("grp"), P("vir")), check_vma=False
    )
```

```python
import jax
import jax.numpy as jnp
from jax import lax
from jax.experimental import pallas as pl
from jax.experimental.pallas import tpu as pltpu
from jax.sharding import PartitionSpec as P

V = 896
BLOCK = 28
ROWS = 32
PAIRS = 15
OW = 5
LEAD = 15
LAG2 = 4
LAG3 = 4
LAG4 = 6
EARLY = 15
CHUNK = 224
NT_DIMS = (((1,), (1,)), ((), ()))


def pair_of(step):
    q = PAIRS - 1 - step
    k = (
        (q >= 1).astype(jnp.int32)
        + (q >= 3).astype(jnp.int32)
        + (q >= 6).astype(jnp.int32)
        + (q >= 10).astype(jnp.int32)
    )
    return q, q - k * (k + 1) // 2, k


def kernel(
    t2_ref, vvvo_ref, hole_hbm, ih_hbm, vir_ref, yc_ref, trips_ref, counts_ref, weights_ref, occ_ref, vsm_ref, pick_ref,
    trip_ref, orb_ref, src, slab, vv, wbuf, th_ref, hole_ref, ih_ref, xb_ref, hit_ref, isem, send1, recv1, send2, recv2, send3, recv3, vsem,
    tile, ybox, part, vbox, ysend, yrecv, psend, precv,
):
    y = lax.axis_index("grp")
    vir = lax.axis_index("vir")
    core = vir % 2
    x = vir // 8
    z = (vir // 2) % 4

    def place(p):
        is_a = (p % 2) == 0
        u = jnp.where(is_a, x, z)
        w = jnp.where(is_a, z, x)
        off = (y + p // 2) % 4
        return is_a, u, w, off

    def device(is_a, u, w):
        return {"vir": jnp.where(is_a, u * 8 + w * 2, w * 8 + u * 2) + core}

    def first(p):
        is_a, u, w, off = place(p)
        return pltpu.make_async_remote_copy(
            src_ref=src.at[p],
            dst_ref=slab.at[p, core, w, :, pl.ds(0, V)],
            send_sem=send1.at[p],
            recv_sem=recv1.at[p],
            device_id=device(is_a, (u + 4 - off) % 4, w),
            device_id_type=pl.DeviceIdType.MESH,
        ), off

    def second(p, turn):
        is_a, u, w, off = place(p)
        shift = (1, 3, 2)[turn]
        return pltpu.make_async_remote_copy(
            src_ref=slab.at[p, core, w, :, pl.ds(0, V)],
            dst_ref=slab.at[p, core, w, :, pl.ds(0, V)],
            send_sem=send2.at[p, turn],
            recv_sem=recv2.at[p, turn],
            device_id=device(is_a, u, (w + shift) % 4),
            device_id_type=pl.DeviceIdType.MESH,
        )

    def relay(p):
        is_a, u, w, off = place(p)
        back = ((p // 2) % 2) == 0
        slot = jnp.where(back, (w + 1) % 4, (w + 3) % 4)
        to = jnp.where(back, (w + 3) % 4, (w + 1) % 4)
        return pltpu.make_async_remote_copy(
            src_ref=slab.at[p, core, slot, :, pl.ds(0, V)],
            dst_ref=slab.at[p, core, slot, :, pl.ds(0, V)],
            send_sem=send2.at[p, 2],
            recv_sem=recv2.at[p, 2],
            device_id=device(is_a, u, to),
            device_id_type=pl.DeviceIdType.MESH,
        )

    def third(p):
        return pltpu.make_async_remote_copy(
            src_ref=slab.at[p, core, :, :, pl.ds(0, V)],
            dst_ref=slab.at[p, core, :, :, pl.ds(0, V)],
            send_sem=send3.at[p],
            recv_sem=recv3.at[p],
            device_id={"vir": vir + 1 - 2 * core},
            device_id_type=pl.DeviceIdType.MESH,
        )

    def load(k):
        return pltpu.make_async_copy(vvvo_ref.at[k], vv.at[k, :, pl.ds(0, V)], vsem.at[k])

    barrier = pltpu.get_barrier_semaphore()

    def greet(r, carry):
        pl.semaphore_signal(
            barrier, inc=1, device_id={"vir": (vir + r) % 32},
            device_id_type=pl.DeviceIdType.MESH)
        return carry

    lax.fori_loop(1, 32, greet, 0)
    for r in (1, 2, 3):
        pl.semaphore_signal(
            barrier, inc=1, device_id={"grp": (y + r) % 4},
            device_id_type=pl.DeviceIdType.MESH)

    holes_in = pltpu.make_async_copy(hole_hbm, hole_ref, isem.at[0])
    ints_in = pltpu.make_async_copy(ih_hbm, ih_ref, isem.at[1])
    holes_in.start()
    ints_in.start()
    load(OW - 1).start()
    for k in range(OW - 2, -1, -1):
        load(k).start()

    def fill(p, carry):
        q, j, k = pair_of(p)
        is_a, u, w, off = place(p)
        block = t2_ref[j, k]
        src[p, BLOCK - 12:, :] = jnp.zeros((ROWS - BLOCK + 12, V), jnp.bfloat16)
        src[p, :BLOCK, :] = block

        @pl.when(off == 0)
        def _():
            slab[p, core, w, BLOCK - 12:, :V] = jnp.zeros((ROWS - BLOCK + 12, V), jnp.bfloat16)
            slab[p, core, w, :BLOCK, :V] = block

        return carry

    lax.fori_loop(0, PAIRS, fill, 0)
    for a in range(2):
        e_a = vsm_ref[pick_ref[a]]
        for c in range(V // 128):
            lines = jnp.broadcast_to(vir_ref[c * 128:(c + 1) * 128][None, :], (128, 128))
            xb_ref[a * V + c * 128:a * V + (c + 1) * 128, :] = lines.T + e_a
    tile[...] = jnp.zeros_like(tile)
    cells = lax.broadcasted_iota(jnp.int32, (1, 128), 1)
    hit_ref[...] = jnp.zeros_like(hit_ref)
    for n in range(6):
        i, j, k = trips_ref[n, 0], trips_ref[n, 1], trips_ref[n, 2]
        code = (k * (k + 1) // 2 + j) * OW + i
        weight = jnp.where(n < counts_ref[0], weights_ref[n], 0).astype(jnp.float32)
        hit_ref[n:n + 1, :] = jnp.where(cells == code, -weight, 0.0) / (V * V)
    tile[2:3, :] = jnp.sum(hit_ref[...], axis=0, keepdims=True)
    pl.semaphore_wait(barrier, 34)

    def start_first(p):
        copy, off = first(p)

        @pl.when(off != 0)
        def _():
            copy.start()

    for p in range(LEAD):
        start_first(p)

    def turn_holes(i):
        for c in range(2 * V // 128):
            at = c * 128
            base = hole_ref[0, :, at:at + 128].astype(jnp.float32)
            this = hole_ref[i, :, at:at + 128].astype(jnp.float32)
            both = jnp.concatenate([base, -this], axis=0)
            th_ref[i, at:at + 128, :] = both.T.astype(jnp.bfloat16)

    def base_holes():
        for c in range(2 * V // 128):
            at = c * 128
            base = hole_ref[0, :, at:at + 128].astype(jnp.float32)
            both = jnp.concatenate([-base, jnp.zeros_like(base)], axis=0)
            turned = both.T.astype(jnp.bfloat16)
            for k in range(OW):
                vv[k, at:at + 128, V:] = turned

    def prepare(p, carry):
        q, j, k = pair_of(p)
        is_a, u, w, off = place(p)
        row = lax.broadcasted_iota(jnp.int32, (256, 1), 0)
        r_core = row // 128
        r_w = (row // ROWS) % 4
        r_in = row % ROWS
        source = (u + off) % 4
        owner = jnp.where(is_a, source * 8 + r_w * 2, r_w * 8 + source * 2) + r_core
        target = jnp.where(r_in < BLOCK, owner * BLOCK + r_in, -1)
        column = lax.broadcasted_iota(jnp.int32, (256, V), 1)
        select = (column == target).astype(jnp.float32).astype(jnp.bfloat16)
        holes = lax.dot_general(
            select, ih_ref[k, j], NT_DIMS, preferred_element_type=jnp.float32
        )
        blank = jnp.zeros((256, 4), jnp.float32)
        holes = jnp.concatenate([holes, blank, holes, blank], axis=1).astype(jnp.bfloat16)
        slab[p, :, :, :, V:] = holes.reshape(2, 4, ROWS, 128)
        return carry

    def compute(p):
        q, j, k = pair_of(p)
        is_a, u, w, off = place(p)
        fresh = (p == 0) | (q == (k + 1) * (k + 2) // 2 - 1)

        @pl.when(fresh)
        def _():
            load(k).wait()

        source = (u + off) % 4
        cols = slab[p].reshape(2 * 4 * ROWS, 1024)
        wbuf[...] = lax.dot_general(vv[k], cols, NT_DIMS, preferred_element_type=jnp.float32)
        holes = slab[p, :, :, :, V:].reshape(256, 128)
        variant = jnp.where(is_a, 0, 4) + source
        yc_row = yc_ref[pl.ds(variant, 1), :]
        lane = lax.broadcasted_iota(jnp.int32, (1, 128), 1)

        def terms(amp, at, yc):
            base = xb_ref[at:at + CHUNK, :]
            den = jnp.concatenate([base, base], axis=1) + yc
            term = amp * amp / den
            return jnp.sum(term.reshape(CHUNK // 8, 8, 256), axis=0)

        def put(total, i, a):
            line = jnp.sum(total, axis=0, keepdims=True)
            line = jnp.sum(line, axis=1, keepdims=True)
            tile[a:a + 1, :] = jnp.where(lane == q * OW + i, line, tile[a:a + 1, :])

        yc = yc_row - (occ_ref[0] + occ_ref[j] + occ_ref[k])
        for a in range(2):
            total = jnp.zeros((8, 256), jnp.float32)
            for c in range(V // CHUNK):
                at = a * V + c * CHUNK
                total = total + terms(wbuf[at:at + CHUNK, :], at, yc)
            put(total, 0, a)

        def one(i, carry):
            yc = yc_row - (occ_ref[i] + occ_ref[j] + occ_ref[k])
            for a in range(2):
                total = jnp.zeros((8, 256), jnp.float32)
                for c in range(V // CHUNK):
                    at = a * V + c * CHUNK
                    hole = lax.dot_general(
                        th_ref[i, at:at + CHUNK, :], holes, NT_DIMS,
                        preferred_element_type=jnp.float32)
                    total = total + terms(wbuf[at:at + CHUNK, :] + hole, at, yc)
                put(total, i, a)
            return carry

        lax.fori_loop(1, j + 1, one, 0)

    def step(s, carry):
        @pl.when(s + LEAD < PAIRS)
        def _():
            start_first(s + LEAD)

        @pl.when(s < PAIRS)
        def _():
            copy, off = first(s)

            @pl.when(off != 0)
            def _():
                copy.wait_recv()

            for turn in range(2):
                second(s, turn).start()

            @pl.when(s < EARLY)
            def _():
                second(s, 2).start()

        @pl.when((s >= LAG2) & (s < PAIRS + LAG2))
        def _():
            for turn in range(2):
                second(s - LAG2, turn).wait_recv()

            @pl.when(s - LAG2 >= EARLY)
            def _():
                relay(s - LAG2).start()

        @pl.when((s >= LAG3) & (s < PAIRS + LAG3))
        def _():
            relay(s - LAG3).wait_recv()
            third(s - LAG3).start()

        @pl.when(s == 0)
        def _():
            ints_in.wait()
            holes_in.wait()
            base_holes()

        @pl.when((s >= 1) & (s < OW))
        def _():
            turn_holes(s)

        @pl.when(s < 5)
        def _():
            lax.fori_loop(3 * s, 3 * s + 3, prepare, 0)

        @pl.when(s >= LAG4)
        def _():
            third(s - LAG4).wait_recv()
            compute(s - LAG4)

        return carry

    lax.fori_loop(0, PAIRS + LAG4, step, 0)

    def drain(p, carry):
        copy, off = first(p)

        @pl.when(off != 0)
        def _():
            copy.wait_send()

        return carry

    def drain_rest(p, carry):
        for turn in range(2):
            second(p, turn).wait_send()
        relay(p).wait_send()
        third(p).wait_send()
        return carry

    lax.fori_loop(0, PAIRS, drain, 0)

    def to_group(r):
        return pltpu.make_async_remote_copy(
            src_ref=tile,
            dst_ref=ybox.at[y],
            send_sem=ysend.at[r - 1],
            recv_sem=yrecv.at[r - 1],
            device_id={"grp": (y + r) % 4},
            device_id_type=pl.DeviceIdType.MESH,
        )

    for r in (1, 2, 3):
        to_group(r).start()
    ybox[y] = tile[...]
    lax.fori_loop(0, PAIRS, drain_rest, 0)
    for r in (1, 2, 3):
        to_group(r).wait_recv()
    whole = ybox[0] + ybox[1] + ybox[2] + ybox[3]
    mine = hit_ref[...] * (whole[0:1, :] + whole[1:2, :])
    part[...] = mine
    vbox[vir] = mine
    orb = jnp.sum(whole[2:3, :] * whole, axis=1, keepdims=True)
    for a in range(2):
        orb_ref[a] = jnp.sum(orb[a:a + 1, :])

    def to_plane(r, carry):
        pltpu.make_async_remote_copy(
            src_ref=part,
            dst_ref=vbox.at[vir],
            send_sem=psend,
            recv_sem=precv,
            device_id={"vir": (vir + r) % 32},
            device_id_type=pl.DeviceIdType.MESH,
        ).start()
        return carry

    lax.fori_loop(1, 32, to_plane, 0)
    for r in (1, 2, 3):
        to_group(r).wait_send()
    others = vbox.at[pl.ds(0, 31)]
    pltpu.make_async_copy(others, others, precv).wait()
    trip = jnp.sum(jnp.sum(vbox[...], axis=0), axis=1, keepdims=True)
    for n in range(6):
        trip_ref[n] = jnp.sum(trip[n:n + 1, :] / 64)
    pltpu.make_async_copy(others, others, psend).wait()


def tables(vir_energy, t2hole):
    split = vir_energy.reshape(4, 4, 2, BLOCK)
    split = jnp.pad(split, ((0, 0), (0, 0), (0, 0), (0, ROWS - BLOCK)), constant_values=1.0)
    by_x = jnp.transpose(split, (0, 2, 1, 3)).reshape(4, 256)
    by_z = jnp.transpose(split, (1, 2, 0, 3)).reshape(4, 256)
    yc = jnp.concatenate([by_x, by_z], axis=0)
    holes = jnp.pad(t2hole.reshape(OW, 60, 2 * V), ((0, 0), (0, 4), (0, 0)))
    return yc, holes


def partial_energies(
    t2pair, ints_vvvo, holes, ints_hole, vir_energy, yc, triplets, counts, weights, occ_energy, a_pick
):
    vmem = pl.BlockSpec(memory_space=pltpu.VMEM)
    smem = pl.BlockSpec(memory_space=pltpu.SMEM)
    hbm = pl.BlockSpec(memory_space=pl.ANY)
    return pl.pallas_call(
        kernel,
        out_shape=[
            jax.ShapeDtypeStruct((6,), jnp.float32), jax.ShapeDtypeStruct((2,), jnp.float32),
        ],
        in_specs=[
            vmem, hbm, hbm, hbm, vmem, vmem, smem, smem, smem, smem, smem, smem,
        ],
        out_specs=[smem, smem],
        scratch_shapes=[
            pltpu.VMEM((PAIRS, ROWS, V), jnp.bfloat16),
            pltpu.VMEM((PAIRS, 2, 4, ROWS, 1024), jnp.bfloat16),
            pltpu.VMEM((OW, 2 * V, 1024), jnp.bfloat16),
            pltpu.VMEM((2 * V, 256), jnp.float32),
            pltpu.VMEM((OW, 2 * V, 128), jnp.bfloat16),
            pltpu.VMEM((OW, 64, 2 * V), jnp.bfloat16),
            pltpu.VMEM((OW, OW, 60, V), jnp.bfloat16),
            pltpu.VMEM((2 * V, 128), jnp.float32),
            pltpu.VMEM((8, 128), jnp.float32),
            pltpu.SemaphoreType.DMA((2,)),
            pltpu.SemaphoreType.DMA((PAIRS,)),
            pltpu.SemaphoreType.DMA((PAIRS,)),
            pltpu.SemaphoreType.DMA((PAIRS, 3)),
            pltpu.SemaphoreType.DMA((PAIRS, 3)),
            pltpu.SemaphoreType.DMA((PAIRS,)),
            pltpu.SemaphoreType.DMA((PAIRS,)),
            pltpu.SemaphoreType.DMA((OW,)),
            pltpu.VMEM((8, 128), jnp.float32),
            pltpu.VMEM((4, 8, 128), jnp.float32),
            pltpu.VMEM((8, 128), jnp.float32),
            pltpu.VMEM((32, 8, 128), jnp.float32),
            pltpu.SemaphoreType.DMA((3,)),
            pltpu.SemaphoreType.DMA((3,)),
            pltpu.SemaphoreType.DMA,
            pltpu.SemaphoreType.DMA,
        ],
        compiler_params=pltpu.CompilerParams(
            collective_id=0, has_side_effects=True, vmem_limit_bytes=60 * 1024 * 1024
        ),
    )(
        t2pair, ints_vvvo.reshape(OW, 2 * V, V), holes, ints_hole,
        vir_energy, yc, triplets, counts, weights, occ_energy, vir_energy, a_pick,
    )


def shards(
    triplets, counts, weights, a_pick, occ_energy, vir_energy, ints_vvvo, t2pair, t2hole, ints_hole
):
    slots = triplets.shape[0]
    yc, holes = tables(vir_energy, t2hole)
    trip, orbital = partial_energies(
        t2pair, ints_vvvo, holes, ints_hole, vir_energy, yc, triplets, counts, weights,
        occ_energy, a_pick,
    )
    return (trip, orbital)


def solution(mesh):
    placed = (
        P("grp", None),
        P("grp"),
        P("grp"),
        P("vir"),
        P(),
        P(),
        P(None, "vir", None, None),
        P(None, None, "vir", None),
        P(None, None, "vir", None),
        P(),
    )
    return jax.shard_map(
        shards, mesh=mesh, in_specs=placed, out_specs=(P("grp"), P("vir")), check_vma=False
    )
```

```python
import jax
import jax.numpy as jnp
from jax import lax
from jax.experimental import pallas as pl
from jax.experimental.pallas import tpu as pltpu
from jax.sharding import PartitionSpec as P

V = 896
BLOCK = 28
ROWS = 32
PAIRS = 15
OW = 5
LEAD = 15
LAG2 = 4
LAG3 = 4
LAG4 = 6
EARLY = 15
CHUNK = 224
NT_DIMS = (((1,), (1,)), ((), ()))


def pair_of(step):
    q = PAIRS - 1 - step
    k = (
        (q >= 1).astype(jnp.int32)
        + (q >= 3).astype(jnp.int32)
        + (q >= 6).astype(jnp.int32)
        + (q >= 10).astype(jnp.int32)
    )
    return q, q - k * (k + 1) // 2, k


def kernel(
    t2_ref, vvvo_ref, hole_hbm, ih_hbm, vir_ref, yc_ref, trips_ref, counts_ref, weights_ref, occ_ref, vsm_ref, pick_ref,
    trip_ref, orb_ref, src, slab, vv, wbuf, th_ref, hole_ref, ih_ref, xb_ref, hit_ref, isem, send1, recv1, send2, recv2, send3, recv3, vsem,
    tile, ybox, part, vbox, ysend, yrecv, psend, precv,
):
    y = lax.axis_index("grp")
    vir = lax.axis_index("vir")
    core = vir % 2
    x = vir // 8
    z = (vir // 2) % 4

    def place(p):
        is_a = (p % 2) == 0
        u = jnp.where(is_a, x, z)
        w = jnp.where(is_a, z, x)
        off = (y + p // 2) % 4
        return is_a, u, w, off

    def device(is_a, u, w):
        return {"vir": jnp.where(is_a, u * 8 + w * 2, w * 8 + u * 2) + core}

    def first(p):
        is_a, u, w, off = place(p)
        return pltpu.make_async_remote_copy(
            src_ref=src.at[p],
            dst_ref=slab.at[p, core, w, :, pl.ds(0, V)],
            send_sem=send1.at[p],
            recv_sem=recv1.at[p],
            device_id=device(is_a, (u + 4 - off) % 4, w),
            device_id_type=pl.DeviceIdType.MESH,
        ), off

    def second(p, turn):
        is_a, u, w, off = place(p)
        shift = (1, 3, 2)[turn]
        return pltpu.make_async_remote_copy(
            src_ref=slab.at[p, core, w, :, pl.ds(0, V)],
            dst_ref=slab.at[p, core, w, :, pl.ds(0, V)],
            send_sem=send2.at[p, turn],
            recv_sem=recv2.at[p, turn],
            device_id=device(is_a, u, (w + shift) % 4),
            device_id_type=pl.DeviceIdType.MESH,
        )

    def relay(p):
        is_a, u, w, off = place(p)
        back = ((p // 2) % 2) == 0
        slot = jnp.where(back, (w + 1) % 4, (w + 3) % 4)
        to = jnp.where(back, (w + 3) % 4, (w + 1) % 4)
        return pltpu.make_async_remote_copy(
            src_ref=slab.at[p, core, slot, :, pl.ds(0, V)],
            dst_ref=slab.at[p, core, slot, :, pl.ds(0, V)],
            send_sem=send2.at[p, 2],
            recv_sem=recv2.at[p, 2],
            device_id=device(is_a, u, to),
            device_id_type=pl.DeviceIdType.MESH,
        )

    def third(p):
        return pltpu.make_async_remote_copy(
            src_ref=slab.at[p, core, :, :, pl.ds(0, V)],
            dst_ref=slab.at[p, core, :, :, pl.ds(0, V)],
            send_sem=send3.at[p],
            recv_sem=recv3.at[p],
            device_id={"vir": vir + 1 - 2 * core},
            device_id_type=pl.DeviceIdType.MESH,
        )

    def load(k):
        return pltpu.make_async_copy(vvvo_ref.at[k], vv.at[k, :, pl.ds(0, V)], vsem.at[k])

    barrier = pltpu.get_barrier_semaphore()

    def greet(r, carry):
        pl.semaphore_signal(
            barrier, inc=1, device_id={"vir": (vir + r) % 32},
            device_id_type=pl.DeviceIdType.MESH)
        return carry

    lax.fori_loop(1, 32, greet, 0)
    for r in (1, 2, 3):
        pl.semaphore_signal(
            barrier, inc=1, device_id={"grp": (y + r) % 4},
            device_id_type=pl.DeviceIdType.MESH)

    holes_in = pltpu.make_async_copy(hole_hbm, hole_ref, isem.at[0])
    ints_in = pltpu.make_async_copy(ih_hbm, ih_ref, isem.at[1])
    holes_in.start()
    ints_in.start()
    load(OW - 1).start()
    for k in range(OW - 2, -1, -1):
        load(k).start()

    def fill(p, carry):
        q, j, k = pair_of(p)
        is_a, u, w, off = place(p)
        block = t2_ref[j, k]
        src[p, BLOCK - 12:, :] = jnp.zeros((ROWS - BLOCK + 12, V), jnp.bfloat16)
        src[p, :BLOCK, :] = block

        @pl.when(off == 0)
        def _():
            slab[p, core, w, BLOCK - 12:, :V] = jnp.zeros((ROWS - BLOCK + 12, V), jnp.bfloat16)
            slab[p, core, w, :BLOCK, :V] = block

        return carry

    lax.fori_loop(0, PAIRS, fill, 0)
    for a in range(2):
        e_a = vsm_ref[pick_ref[a]]
        for c in range(V // 128):
            lines = jnp.broadcast_to(vir_ref[c * 128:(c + 1) * 128][None, :], (128, 128))
            xb_ref[a * V + c * 128:a * V + (c + 1) * 128, :] = lines.T + e_a
    tile[...] = jnp.zeros_like(tile)
    cells = lax.broadcasted_iota(jnp.int32, (1, 128), 1)
    hit_ref[...] = jnp.zeros_like(hit_ref)
    for n in range(6):
        i, j, k = trips_ref[n, 0], trips_ref[n, 1], trips_ref[n, 2]
        code = (k * (k + 1) // 2 + j) * OW + i
        weight = jnp.where(n < counts_ref[0], weights_ref[n], 0).astype(jnp.float32)
        hit_ref[n:n + 1, :] = jnp.where(cells == code, -weight, 0.0) / (V * V)
    tile[2:3, :] = jnp.sum(hit_ref[...], axis=0, keepdims=True)
    pl.semaphore_wait(barrier, 34)

    def start_first(p):
        copy, off = first(p)

        @pl.when(off != 0)
        def _():
            copy.start()

    for p in range(LEAD):
        start_first(p)

    def read_holes(i, a, at):
        some = hole_ref[i, :, :, at:at + 128].astype(jnp.float32)[:, a, :]
        return jnp.concatenate([some, jnp.zeros((4, 128), jnp.float32)], axis=0)

    def turn_holes(c):
        a, at = c // 7, (c % 7) * 128
        row = c * 128
        base = read_holes(0, a, at)
        both = jnp.concatenate([-base, jnp.zeros_like(base)], axis=0)
        turned = both.T.astype(jnp.bfloat16)
        for k in range(OW):
            vv[k, row:row + 128, V:] = turned
        for i in range(1, OW):
            both = jnp.concatenate([base, -read_holes(i, a, at)], axis=0)
            th_ref[i, row:row + 128, :] = both.T.astype(jnp.bfloat16)

    def prepare(p, carry):
        q, j, k = pair_of(p)
        is_a, u, w, off = place(p)
        row = lax.broadcasted_iota(jnp.int32, (256, 1), 0)
        r_core = row // 128
        r_w = (row // ROWS) % 4
        r_in = row % ROWS
        source = (u + off) % 4
        owner = jnp.where(is_a, source * 8 + r_w * 2, r_w * 8 + source * 2) + r_core
        target = jnp.where(r_in < BLOCK, owner * BLOCK + r_in, -1)
        column = lax.broadcasted_iota(jnp.int32, (256, V), 1)
        select = (column == target).astype(jnp.float32).astype(jnp.bfloat16)
        holes = lax.dot_general(
            select, ih_ref[k, j], NT_DIMS, preferred_element_type=jnp.float32
        )
        blank = jnp.zeros((256, 4), jnp.float32)
        holes = jnp.concatenate([holes, blank, holes, blank], axis=1).astype(jnp.bfloat16)
        slab[p, :, :, :, V:] = holes.reshape(2, 4, ROWS, 128)
        return carry

    def compute(p):
        q, j, k = pair_of(p)
        is_a, u, w, off = place(p)
        fresh = (p == 0) | (q == (k + 1) * (k + 2) // 2 - 1)

        @pl.when(fresh)
        def _():
            load(k).wait()

        source = (u + off) % 4
        cols = slab[p].reshape(2 * 4 * ROWS, 1024)
        wbuf[...] = lax.dot_general(vv[k], cols, NT_DIMS, preferred_element_type=jnp.float32)
        holes = slab[p, :, :, :, V:].reshape(256, 128)
        variant = jnp.where(is_a, 0, 4) + source
        yc_row = yc_ref[pl.ds(variant, 1), :]
        lane = lax.broadcasted_iota(jnp.int32, (1, 128), 1)

        def terms(amp, at, yc):
            base = xb_ref[at:at + CHUNK, :]
            den = jnp.concatenate([base, base], axis=1) + yc
            term = amp * amp / den
            return jnp.sum(term.reshape(CHUNK // 8, 8, 256), axis=0)

        def put(total, i, a):
            line = jnp.sum(total, axis=0, keepdims=True)
            line = jnp.sum(line, axis=1, keepdims=True)
            tile[a:a + 1, :] = jnp.where(lane == q * OW + i, line, tile[a:a + 1, :])

        yc = yc_row - (occ_ref[0] + occ_ref[j] + occ_ref[k])
        for a in range(2):
            total = jnp.zeros((8, 256), jnp.float32)
            for c in range(V // CHUNK):
                at = a * V + c * CHUNK
                total = total + terms(wbuf[at:at + CHUNK, :], at, yc)
            put(total, 0, a)

        def one(i, carry):
            yc = yc_row - (occ_ref[i] + occ_ref[j] + occ_ref[k])
            for a in range(2):
                total = jnp.zeros((8, 256), jnp.float32)
                for c in range(V // CHUNK):
                    at = a * V + c * CHUNK
                    hole = lax.dot_general(
                        th_ref[i, at:at + CHUNK, :], holes, NT_DIMS,
                        preferred_element_type=jnp.float32)
                    total = total + terms(wbuf[at:at + CHUNK, :] + hole, at, yc)
                put(total, i, a)
            return carry

        lax.fori_loop(1, j + 1, one, 0)

    def step(s, carry):
        @pl.when(s + LEAD < PAIRS)
        def _():
            start_first(s + LEAD)

        @pl.when(s < PAIRS)
        def _():
            copy, off = first(s)

            @pl.when(off != 0)
            def _():
                copy.wait_recv()

            for turn in range(2):
                second(s, turn).start()

            @pl.when(s < EARLY)
            def _():
                second(s, 2).start()

        @pl.when((s >= LAG2) & (s < PAIRS + LAG2))
        def _():
            for turn in range(2):
                second(s - LAG2, turn).wait_recv()

            @pl.when(s - LAG2 >= EARLY)
            def _():
                relay(s - LAG2).start()

        @pl.when((s >= LAG3) & (s < PAIRS + LAG3))
        def _():
            relay(s - LAG3).wait_recv()
            third(s - LAG3).start()

        @pl.when(s == 0)
        def _():
            ints_in.wait()
            holes_in.wait()

        for part_at in range(5):
            @pl.when(s == part_at)
            def _():
                for c in range(3 * part_at, min(14, 3 * part_at + 3)):
                    turn_holes(c)

        @pl.when(s < 5)
        def _():
            lax.fori_loop(3 * s, 3 * s + 3, prepare, 0)

        @pl.when(s >= LAG4)
        def _():
            third(s - LAG4).wait_recv()
            compute(s - LAG4)

        return carry

    lax.fori_loop(0, PAIRS + LAG4, step, 0)

    def drain(p, carry):
        copy, off = first(p)

        @pl.when(off != 0)
        def _():
            copy.wait_send()

        return carry

    def drain_rest(p, carry):
        for turn in range(2):
            second(p, turn).wait_send()
        relay(p).wait_send()
        third(p).wait_send()
        return carry

    lax.fori_loop(0, PAIRS, drain, 0)

    def to_group(r):
        return pltpu.make_async_remote_copy(
            src_ref=tile,
            dst_ref=ybox.at[y],
            send_sem=ysend.at[r - 1],
            recv_sem=yrecv.at[r - 1],
            device_id={"grp": (y + r) % 4},
            device_id_type=pl.DeviceIdType.MESH,
        )

    for r in (1, 2, 3):
        to_group(r).start()
    ybox[y] = tile[...]
    lax.fori_loop(0, PAIRS, drain_rest, 0)
    for r in (1, 2, 3):
        to_group(r).wait_recv()
    whole = ybox[0] + ybox[1] + ybox[2] + ybox[3]
    mine = hit_ref[...] * (whole[0:1, :] + whole[1:2, :])
    part[...] = mine
    vbox[vir] = mine
    orb = jnp.sum(whole[2:3, :] * whole, axis=1, keepdims=True)
    for a in range(2):
        orb_ref[a] = jnp.sum(orb[a:a + 1, :])

    def to_plane(r, carry):
        pltpu.make_async_remote_copy(
            src_ref=part,
            dst_ref=vbox.at[vir],
            send_sem=psend,
            recv_sem=precv,
            device_id={"vir": (vir + r) % 32},
            device_id_type=pl.DeviceIdType.MESH,
        ).start()
        return carry

    lax.fori_loop(1, 32, to_plane, 0)
    for r in (1, 2, 3):
        to_group(r).wait_send()
    others = vbox.at[pl.ds(0, 31)]
    pltpu.make_async_copy(others, others, precv).wait()
    trip = jnp.sum(jnp.sum(vbox[...], axis=0), axis=1, keepdims=True)
    for n in range(6):
        trip_ref[n] = jnp.sum(trip[n:n + 1, :] / 64)
    pltpu.make_async_copy(others, others, psend).wait()


def tables(vir_energy):
    split = vir_energy.reshape(4, 4, 2, BLOCK)
    split = jnp.pad(split, ((0, 0), (0, 0), (0, 0), (0, ROWS - BLOCK)), constant_values=1.0)
    by_x = jnp.transpose(split, (0, 2, 1, 3)).reshape(4, 256)
    by_z = jnp.transpose(split, (1, 2, 0, 3)).reshape(4, 256)
    yc = jnp.concatenate([by_x, by_z], axis=0)
    return yc


def partial_energies(
    t2pair, ints_vvvo, holes, ints_hole, vir_energy, yc, triplets, counts, weights, occ_energy, a_pick
):
    vmem = pl.BlockSpec(memory_space=pltpu.VMEM)
    smem = pl.BlockSpec(memory_space=pltpu.SMEM)
    hbm = pl.BlockSpec(memory_space=pl.ANY)
    return pl.pallas_call(
        kernel,
        out_shape=[
            jax.ShapeDtypeStruct((6,), jnp.float32), jax.ShapeDtypeStruct((2,), jnp.float32),
        ],
        in_specs=[
            vmem, hbm, hbm, hbm, vmem, vmem, smem, smem, smem, smem, smem, smem,
        ],
        out_specs=[smem, smem],
        scratch_shapes=[
            pltpu.VMEM((PAIRS, ROWS, V), jnp.bfloat16),
            pltpu.VMEM((PAIRS, 2, 4, ROWS, 1024), jnp.bfloat16),
            pltpu.VMEM((OW, 2 * V, 1024), jnp.bfloat16),
            pltpu.VMEM((2 * V, 256), jnp.float32),
            pltpu.VMEM((OW, 2 * V, 128), jnp.bfloat16),
            pltpu.VMEM((OW, 60, 2, V), jnp.bfloat16),
            pltpu.VMEM((OW, OW, 60, V), jnp.bfloat16),
            pltpu.VMEM((2 * V, 128), jnp.float32),
            pltpu.VMEM((8, 128), jnp.float32),
            pltpu.SemaphoreType.DMA((2,)),
            pltpu.SemaphoreType.DMA((PAIRS,)),
            pltpu.SemaphoreType.DMA((PAIRS,)),
            pltpu.SemaphoreType.DMA((PAIRS, 3)),
            pltpu.SemaphoreType.DMA((PAIRS, 3)),
            pltpu.SemaphoreType.DMA((PAIRS,)),
            pltpu.SemaphoreType.DMA((PAIRS,)),
            pltpu.SemaphoreType.DMA((OW,)),
            pltpu.VMEM((8, 128), jnp.float32),
            pltpu.VMEM((4, 8, 128), jnp.float32),
            pltpu.VMEM((8, 128), jnp.float32),
            pltpu.VMEM((32, 8, 128), jnp.float32),
            pltpu.SemaphoreType.DMA((3,)),
            pltpu.SemaphoreType.DMA((3,)),
            pltpu.SemaphoreType.DMA,
            pltpu.SemaphoreType.DMA,
        ],
        compiler_params=pltpu.CompilerParams(
            collective_id=0, has_side_effects=True, vmem_limit_bytes=60 * 1024 * 1024
        ),
    )(
        t2pair, ints_vvvo.reshape(OW, 2 * V, V), holes, ints_hole,
        vir_energy, yc, triplets, counts, weights, occ_energy, vir_energy, a_pick,
    )


def shards(
    triplets, counts, weights, a_pick, occ_energy, vir_energy, ints_vvvo, t2pair, t2hole, ints_hole
):
    slots = triplets.shape[0]
    yc = tables(vir_energy)
    trip, orbital = partial_energies(
        t2pair, ints_vvvo, t2hole, ints_hole, vir_energy, yc, triplets, counts, weights,
        occ_energy, a_pick,
    )
    return (trip, orbital)


def solution(mesh):
    placed = (
        P("grp", None),
        P("grp"),
        P("grp"),
        P("vir"),
        P(),
        P(),
        P(None, "vir", None, None),
        P(None, None, "vir", None),
        P(None, None, "vir", None),
        P(),
    )
    return jax.shard_map(
        shards, mesh=mesh, in_specs=placed, out_specs=(P("grp"), P("vir")), check_vma=False
    )
```
